32 devices in a mesh: data: 2 (over x), ctxo: 4 (over z), ctx: 4 (over y, core).
Axes of the slice: x: 2, y: 2, z: 4, core: 2. Of those that a mesh axis runs over, the one named last changes fastest.
Arguments:
- q_seq: bfloat16 [4, 6144, 7, 128], P('data', ('ctxo', 'ctx')), parts along dimension 0
- k_seq: bfloat16 [4, 6144, 1, 128], P('data', ('ctxo', 'ctx')), parts along dimension 0
- v_seq: bfloat16 [4, 6144, 1, 128], P('data', ('ctxo', 'ctx')), parts along dimension 0
- do_seq: bfloat16 [4, 6144, 7, 128], P('data', ('ctxo', 'ctx')), parts along dimension 0
Outputs:
- output 1: bfloat16 [4, 6144, 7, 128], P('data', ('ctxo', 'ctx')), parts along dimension 0
- output 2: bfloat16 [4, 6144, 7, 128], P('data', ('ctxo', 'ctx')), parts along dimension 0
- output 3: bfloat16 [4, 6144, 1, 128], P('data', ('ctxo', 'ctx')), parts along dimension 0
- output 4: bfloat16 [4, 6144, 1, 128], P('data', ('ctxo', 'ctx')), parts along dimension 0
There are 2 independent parts. The reference program is written for one: setup_inputs(seed, part) draws one part's arguments, and reference() takes and returns one part's arrays. A program takes and returns all parts, laid end to end along the dimension named above; each array names one.
All inputs are finite; a program needn't handle non-finite values.
Results may differ from the reference program's by a relative error of at most 0.0126409.
Values are sent between devices in bfloat16 or wider.
A program may use at most 1 GiB of HBM per device.

```python
import math
import jax
import jax.numpy as jnp
from jax import lax

BATCH_SEQS = 2
SEQ_LEN = 6144
Q_LOCAL = 7
KV_LOCAL = 1
HEAD_DIM = 128
ROW_BLOCK = 64


def setup_inputs(seed: int = 0, part: int = 0) -> dict:
    base_key = jax.random.fold_in(jax.random.key(seed), part)
    key_q, key_k, key_v, key_d = jax.random.split(base_key, 4)
    q_shape = (BATCH_SEQS, SEQ_LEN, Q_LOCAL, HEAD_DIM)
    kv_shape = (BATCH_SEQS, SEQ_LEN, KV_LOCAL, HEAD_DIM)
    spread = math.sqrt(1.0 + math.log(max(SEQ_LEN / 256.0, 1.0)))
    q_seq = spread * jax.random.normal(key_q, q_shape, jnp.float32)
    k_seq = jax.random.normal(key_k, kv_shape, jnp.float32)
    v_seq = jax.random.normal(key_v, kv_shape, jnp.float32)
    do_seq = jax.random.normal(key_d, q_shape, jnp.float32)
    return {'q_seq': q_seq.astype(jnp.bfloat16), 'k_seq': k_seq.astype(jnp.bfloat16), 'v_seq': v_seq.astype(jnp.bfloat16), 'do_seq': do_seq.astype(jnp.bfloat16)}


def reference(q_seq, k_seq, v_seq, do_seq):
    group_size = Q_LOCAL // KV_LOCAL
    n_blocks = SEQ_LEN // ROW_BLOCK
    q_scale = 1.0 / math.sqrt(HEAD_DIM)
    blocked = (BATCH_SEQS, n_blocks, ROW_BLOCK, KV_LOCAL, group_size, HEAD_DIM)
    q_rows = jnp.moveaxis(q_seq.astype(jnp.float32).reshape(blocked), 1, 0)
    do_rows = jnp.moveaxis(do_seq.astype(jnp.float32).reshape(blocked), 1, 0)
    key_pos = lax.broadcasted_iota(jnp.int32, (1, 1, SEQ_LEN), 2)
    row_pos = lax.broadcasted_iota(jnp.int32, (ROW_BLOCK, 1, 1), 0)

    def attention(q_blocks, keys_all, vals_all):
        def one_block(block_in):
            q_blk, blk_idx = block_in
            scores = jnp.einsum('bqhgd,bkhd->bhqgk', q_blk, keys_all) * q_scale
            visible = row_pos + blk_idx * ROW_BLOCK >= key_pos
            probs_blk = jax.nn.softmax(jnp.where(visible, scores, -jnp.inf), axis=-1)
            return jnp.einsum('bhqgk,bkhd->bqhgd', probs_blk, vals_all)
        return lax.map(jax.checkpoint(one_block), (q_blocks, jnp.arange(n_blocks)))

    out_rows, pull_back = jax.vjp(attention, q_rows, k_seq.astype(jnp.float32), v_seq.astype(jnp.float32))
    dq_rows, dk_all, dv_all = pull_back(do_rows)
    q_full = (BATCH_SEQS, SEQ_LEN, Q_LOCAL, HEAD_DIM)
    out_seq = jnp.moveaxis(out_rows, 0, 1).reshape(q_full)
    dq_seq = jnp.moveaxis(dq_rows, 0, 1).reshape(q_full)
    return (out_seq.astype(jnp.bfloat16), dq_seq.astype(jnp.bfloat16), dk_all.astype(jnp.bfloat16), dv_all.astype(jnp.bfloat16))
```

```python
import functools
import math

import jax
import jax.numpy as jnp
from jax import lax
from jax.experimental import pallas as pl
from jax.experimental.pallas import tpu as pltpu
from jax.sharding import PartitionSpec as P

MESH = pl.DeviceIdType.MESH
BF = jnp.bfloat16
F32 = jnp.float32


def dot(a, b):
    return jnp.dot(a, b, preferred_element_type=F32)


def kernel(nz, q_in, do_in, k_in, v_in, o_out, dq_out, dk_out, dv_out,
           qs, dos, qT, doT, kvs, kT, vT, oT, dqT, mr, lr, dr, sb, mbr, dkv, ybuf, zbuf, os, dqs, gs,
           in_loc, in_snd, in_rcv, kv_zs, kv_fs, kv_rcv, y_snd, y_rcv, z_snd, z_rcv,
           o_loc, o_snd, o_rcv, g_loc, g_snd, g_rcv, dq_loc, dq_snd, dq_rcv):
    heads, chip_len, dim = qs.shape
    half = chip_len // 2
    tile = min(256, chip_len)
    n_tiles = chip_len // tile
    scale = 1.0 / math.sqrt(dim)
    c2 = scale * math.log2(math.e)

    z = lax.axis_index("ctxo")
    x = lax.axis_index("ctx")
    m = lax.rem(x, 2)
    y = x // 2
    c = 2 * z + y
    peer = {"ctx": 2 * y + 1 - m}
    yn = {"ctx": 2 * (1 - y) + m}
    my_rows = pl.ds(pl.multiple_of(m * half, half), half)
    peer_rows = pl.ds(pl.multiple_of((1 - m) * half, half), half)

    def rcopy(src, dst, ss, rs, dev):
        return pltpu.make_async_remote_copy(src_ref=src, dst_ref=dst, send_sem=ss, recv_sem=rs, device_id=dev, device_id_type=MESH)

    bar = pltpu.get_barrier_semaphore()
    pl.semaphore_signal(bar, inc=1, device_id=peer, device_id_type=MESH)
    pl.semaphore_signal(bar, inc=1, device_id=yn, device_id_type=MESH)
    for d in range(1, nz):
        pl.semaphore_signal(bar, inc=1, device_id={"ctxo": lax.rem(z + d, nz)}, device_id_type=MESH)
    pl.semaphore_wait(bar, nz + 1)

    ins = ((k_in, kvs.at[c, 0]), (v_in, kvs.at[c, 1]), (q_in, qs), (do_in, dos))
    loc, rem = [], []
    for i, (src, dst) in enumerate(ins):
        d = dst.at[my_rows] if i < 2 else dst.at[:, my_rows]
        rem.append(rcopy(src.at[1 - m], d, in_snd.at[i], in_rcv.at[i], peer))
        loc.append(pltpu.make_async_copy(src.at[m], d, in_loc.at[i]))
        rem[-1].start()
        loc[-1].start()
    for i in (0, 1):
        loc[i].wait()
        rem[i].wait_recv()

    def kv_z(t):
        return rcopy(kvs.at[c], kvs.at[c], kv_zs.at[t], kv_rcv.at[c], {"ctxo": t})

    def kv_fwd(p):
        b = 2 * p + y
        return rcopy(kvs.at[b], kvs.at[b], kv_fs.at[p], kv_rcv.at[b], yn)

    def kv_wait(b):
        rcopy(kvs.at[b], kvs.at[b], kv_fs.at[0], kv_rcv.at[b], yn).wait_recv()

    for t in range(nz - 1, 0, -1):
        @pl.when(z < t)
        def _():
            kv_z(t).start()

    @pl.when(y == 0)
    def _():
        kv_fwd(z).start()

    def prep_kv(b):
        kT[b] = kvs[b, 0].T
        vT[b] = kvs[b, 1].T

    prep_kv(c)
    for i in (2, 3):
        loc[i].wait()
        rem[i].wait_recv()

    def prep_q(h, _):
        qT[h] = qs[h].T
        doT[h] = dos[h].T
        return 0

    lax.fori_loop(0, heads, prep_q, 0)

    def tri():
        r = lax.broadcasted_iota(jnp.int32, (tile, tile), 0)
        s = lax.broadcasted_iota(jnp.int32, (tile, tile), 1)
        return s >= r

    def span(t, diag):
        return (t + 1) * tile if diag else chip_len

    def cols(t):
        return slice(t * tile, (t + 1) * tile)

    def masked(s, nk, fill):
        low = jnp.where(tri(), s[nk - tile:], fill)
        return jnp.concatenate([s[:nk - tile], low], axis=0) if nk > tile else low

    def put_scores(t, diag, s):
        nk = span(t, diag)
        if diag:
            s = masked(s, nk, -jnp.inf)
        sb[:nk, cols(t)] = s
        mbr[:, cols(t)] = jnp.max(s, axis=0, keepdims=True)

    def scores(b, h, t, diag):
        return dot(kvs[b, 0, :span(t, diag), :], qT[h, :, cols(t)])

    def fwd_step(b, h, diag, bn, hn, diag_n):
        for t in range(n_tiles):
            sl = cols(t)
            nk = span(t, diag)
            top = mbr[:, sl]
            if not diag:
                old = mr[h, :, sl]
                top = jnp.maximum(old, top)
                fade = jnp.exp2((old - top) * c2)
            s = sb[:nk, sl]
            sn = scores(bn, hn, t, diag_n)
            p = jnp.exp2((s - top) * c2)
            tot = jnp.sum(p, axis=0, keepdims=True)
            o = dot(vT[b, :, :nk], p.astype(BF))
            put_scores(t, diag_n, sn)
            if diag:
                lr[h, :, sl] = tot
                oT[h, :, sl] = o
            else:
                lr[h, :, sl] = lr[h, :, sl] * fade + tot
                oT[h, :, sl] = oT[h, :, sl] * fade + o
            mr[h, :, sl] = top

    def fwd_block(i):
        k = jnp.maximum(i - y, 0)
        p = jnp.maximum(z - 1 - k // 2, 0)
        b = 2 * p + jnp.where(lax.rem(k, 2) == 0, y, 1 - y)
        b = jnp.where(jnp.logical_and(y == 1, i == 0), 2 * z, b)
        return jnp.where(i >= c, c, b)

    def arrive(i):
        k = i - y
        b = fwd_block(i)

        @pl.when(jnp.logical_and(k >= 0, k < 2 * z))
        def _():
            p = z - 1 - k // 2

            @pl.when(jnp.logical_and(k == 0, z > 0))
            def _():
                kv_wait(2 * p + y)
                kv_fwd(p).start()

            @pl.when(lax.rem(k, 2) == 1)
            def _():
                @pl.when(p > 0)
                def _():
                    kv_wait(2 * p - 2 + y)
                    kv_fwd(p - 1).start()

                kv_wait(b)

        @pl.when(jnp.logical_and(k < 0, c > 0))
        def _():
            kv_wait(b)

        @pl.when(i < c)
        def _():
            prep_kv(b)

    for t in range(n_tiles):
        put_scores(t, True, scores(c, 0, t, True))

    def fwd_diag(h, _):
        fwd_step(c, h, True, c, h + 1, True)
        return 0

    lax.fori_loop(0, heads - 1, fwd_diag, 0)
    arrive(0)
    fwd_step(c, heads - 1, True, fwd_block(0), 0, False)

    def fwd_full(n, _):
        i = n // heads
        h = n - i * heads
        last = h == heads - 1

        @pl.when(last)
        def _():
            arrive(i + 1)

        fwd_step(fwd_block(i), h, False, fwd_block(jnp.where(last, i + 1, i)), jnp.where(last, 0, h + 1), False)
        return 0

    lax.fori_loop(0, c * heads, fwd_full, 0)

    def fwd_end(h, _):
        l = lr[h]
        o = oT[h] / l
        mr[h] = mr[h] * c2 + jnp.log2(l)
        dr[h] = jnp.sum(o * doT[h].astype(F32), axis=0, keepdims=True)
        os[h] = o.T.astype(BF)
        dqT[h] = jnp.zeros_like(o)
        return 0

    lax.fori_loop(0, heads, fwd_end, 0)

    def bwd_step(b, h, diag):
        for t in range(n_tiles):
            sl = cols(t)
            nk = span(t, diag)
            s = dot(kvs[b, 0, :nk, :], qT[h, :, sl])
            dp = dot(kvs[b, 1, :nk, :], doT[h, :, sl])
            p = jnp.exp2(s * c2 - mr[h, :, sl])
            if diag:
                p = masked(p, nk, 0.0)
            ds = (p * (dp - dr[h, :, sl])).astype(BF)
            dkv[b, 1, :nk, :] += dot(p.astype(BF), dos[h, sl, :])
            dkv[b, 0, :nk, :] += dot(ds, qs[h, sl, :])
            dqT[h, :, sl] += dot(kT[b, :, :nk], ds)

    def o_copies():
        return (pltpu.make_async_copy(os.at[:, my_rows], o_out.at[m], o_loc),
                rcopy(os.at[:, peer_rows], o_out.at[m], o_snd, o_rcv, peer))

    def bwd_block(i):
        p = i // 2
        b = 2 * p + jnp.where(lax.rem(i, 2) == 0, 1 - y, y)
        return jnp.where(i >= 2 * z, 2 * z, b)

    def y_send(p):
        return rcopy(dkv.at[2 * p + 1 - y], ybuf.at[p], y_snd.at[p], y_rcv.at[p], yn)

    def z_send(p):
        return rcopy(dkv.at[2 * p + y], zbuf.at[z], z_snd.at[p], z_rcv.at[z], {"ctxo": p})

    def y_wait(p):
        rcopy(dkv.at[0], ybuf.at[p], y_snd.at[p], y_rcv.at[p], yn).wait_recv()

    def combine(p):
        y_wait(p)
        dkv[2 * p + y] = dkv[2 * p + y] + ybuf[p]
        z_send(p).start()

    def bwd_full(i, _):
        b = bwd_block(i)
        dkv[b] = jnp.zeros_like(dkv[b])

        def one(h, _):
            bwd_step(b, h, False)
            return 0

        lax.fori_loop(0, heads, one, 0)

        @pl.when(jnp.logical_or(lax.rem(i, 2) == 0, i >= 2 * z))
        def _():
            y_send(i // 2).start()

        @pl.when(jnp.logical_and(lax.rem(i, 2) == 0, i > 0))
        def _():
            combine(i // 2 - 1)

        @pl.when(i == 0)
        def _():
            for cp in o_copies():
                cp.start()

        return 0

    lax.fori_loop(0, c, bwd_full, 0)

    @pl.when(c == 0)
    def _():
        for cp in o_copies():
            cp.start()

    dkv[c] = jnp.zeros_like(dkv[c])

    def dq_copies(h):
        return (pltpu.make_async_copy(dqs.at[h, my_rows], dq_out.at[m, h], dq_loc.at[h]),
                rcopy(dqs.at[h, peer_rows], dq_out.at[m, h], dq_snd.at[h], dq_rcv.at[h], peer))

    def bwd_diag(h, _):
        bwd_step(c, h, True)
        dqs[h] = (dqT[h] * scale).T.astype(BF)

        @pl.when(h > 0)
        def _():
            for cp in dq_copies(h - 1):
                cp.start()

        return 0

    lax.fori_loop(0, heads, bwd_diag, 0)
    for cp in dq_copies(heads - 1):
        cp.start()

    @pl.when(jnp.logical_and(y == 0, z > 0))
    def _():
        combine(z - 1)

    for t in range(nz - 1, 0, -1):
        @pl.when(z < t)
        def _():
            rcopy(dkv.at[0], zbuf.at[t], z_snd.at[0], z_rcv.at[t], {"ctxo": t}).wait_recv()
            dkv[c] = dkv[c] + zbuf[t]

    @pl.when(y == 0)
    def _():
        y_wait(z)
        dkv[c] = dkv[c] + ybuf[z]

    gs[0] = (dkv[c, 0] * scale).astype(BF)
    gs[1] = dkv[c, 1].astype(BF)
    outs = (dk_out, dv_out)
    g_copies = []
    for i in (0, 1):
        g_copies.append((pltpu.make_async_copy(gs.at[i, my_rows], outs[i].at[m], g_loc.at[i]),
                         rcopy(gs.at[i, peer_rows], outs[i].at[m], g_snd.at[i], g_rcv.at[i], peer)))
        for cp in g_copies[-1]:
            cp.start()

    for i in range(4):
        rem[i].wait_send()
    for t in range(1, nz):
        @pl.when(z < t)
        def _():
            kv_z(t).wait_send()
    for p in range(nz):
        @pl.when(jnp.logical_or(p < z, jnp.logical_and(p == z, y == 0)))
        def _():
            kv_fwd(p).wait_send()

        @pl.when(jnp.logical_or(p < z, jnp.logical_and(p == z, y == 1)))
        def _():
            y_send(p).wait_send()

        @pl.when(p < z)
        def _():
            z_send(p).wait_send()
    a, b = o_copies()
    a.wait()
    b.wait()
    for h in range(heads):
        a, b = dq_copies(h)
        a.wait()
        b.wait()
    for a, b in g_copies:
        a.wait()
        b.wait()


def solution(mesh):
    nz = mesh.shape["ctxo"]
    spec = P("data", ("ctxo", "ctx"), None, None)

    def local(q, k, v, do):
        rows, half, heads, dim = q.shape
        n = 2 * half
        nb = 2 * nz
        q, do = jnp.swapaxes(q, 1, 2), jnp.swapaxes(do, 1, 2)
        k, v = k[:, :, 0], v[:, :, 0]
        hbm = pl.BlockSpec(memory_space=pl.ANY)
        dma = pltpu.SemaphoreType.DMA
        S = jax.ShapeDtypeStruct
        V = pltpu.VMEM
        o, dq, dk, dv = pl.pallas_call(
            functools.partial(kernel, nz),
            out_shape=[S(q.shape, BF), S(q.shape, BF), S(k.shape, BF), S(k.shape, BF)],
            in_specs=[hbm] * 4,
            out_specs=[hbm] * 4,
            scratch_shapes=[
                V((heads, n, dim), BF), V((heads, n, dim), BF), V((heads, dim, n), BF), V((heads, dim, n), BF),
                V((nb, 2, n, dim), BF), V((nb, dim, n), BF), V((nb, dim, n), BF),
                V((heads, dim, n), F32), V((heads, dim, n), F32),
                V((heads, 1, n), F32), V((heads, 1, n), F32), V((heads, 1, n), F32),
                V((n, n), F32), V((1, n), F32),
                V((nb, 2, n, dim), F32), V((nz, 2, n, dim), F32), V((nz, 2, n, dim), F32),
                V((heads, n, dim), BF), V((heads, n, dim), BF), V((2, n, dim), BF),
                dma((4,)), dma((4,)), dma((4,)), dma((nz,)), dma((nz,)), dma((nb,)),
                dma((nz,)), dma((nz,)), dma((nz,)), dma((nz,)),
                dma, dma, dma, dma((2,)), dma((2,)), dma((2,)), dma((heads,)), dma((heads,)), dma((heads,)),
            ],
            compiler_params=pltpu.CompilerParams(collective_id=0, has_side_effects=True, vmem_limit_bytes=62 * 1024 * 1024),
            name="attn",
        )(q, do, k, v)
        return jnp.swapaxes(o, 1, 2), jnp.swapaxes(dq, 1, 2), dk[:, :, None], dv[:, :, None]

    return jax.shard_map(local, mesh=mesh, in_specs=(spec,) * 4, out_specs=(spec,) * 4, check_vma=False)
```

```python
import functools
import math

import jax
import jax.numpy as jnp
from jax import lax
from jax.experimental import pallas as pl
from jax.experimental.pallas import tpu as pltpu
from jax.sharding import PartitionSpec as P

MESH = pl.DeviceIdType.MESH
BF = jnp.bfloat16
F32 = jnp.float32
DIAG, SIB, FULL = 0, 1, 2


def dot(a, b):
    return jnp.dot(a, b, preferred_element_type=F32)


def kernel(nz, q_in, do_in, k_in, v_in, o_out, dq_out, dk_out, dv_out,
           qs, dos, qT, doT, kvs, kT, vT, oT, dqT, mr, lr, dr, sb, mbr, dkv, ybuf, zbuf, os, dqs, gs,
           in_loc, in_snd, in_rcv, kv_zs, kv_fs, kv_rcv, y_snd, y_rcv, z_snd, z_rcv,
           o_loc, o_snd, o_rcv, g_loc, g_snd, g_rcv, dq_loc, dq_snd, dq_rcv):
    heads, chip_len, dim = qs.shape
    half = chip_len // 2
    tile = min(256, chip_len)
    n_tiles = chip_len // tile
    scale = 1.0 / math.sqrt(dim)
    c2 = scale * math.log2(math.e)

    z = lax.axis_index("ctxo")
    x = lax.axis_index("ctx")
    m = lax.rem(x, 2)
    y = x // 2
    c = 2 * z + m
    peer = {"ctx": 2 * (1 - y) + m}
    sib = {"ctx": 2 * y + 1 - m}
    my_rows = pl.ds(pl.multiple_of(y * half, half), half)
    peer_rows = pl.ds(pl.multiple_of((1 - y) * half, half), half)

    def rcopy(src, dst, ss, rs, dev):
        return pltpu.make_async_remote_copy(src_ref=src, dst_ref=dst, send_sem=ss, recv_sem=rs, device_id=dev, device_id_type=MESH)

    bar = pltpu.get_barrier_semaphore()
    pl.semaphore_signal(bar, inc=1, device_id=peer, device_id_type=MESH)
    pl.semaphore_signal(bar, inc=1, device_id=sib, device_id_type=MESH)
    for d in range(1, nz):
        pl.semaphore_signal(bar, inc=1, device_id={"ctxo": lax.rem(z + d, nz)}, device_id_type=MESH)
    pl.semaphore_wait(bar, nz + 1)

    rem, loc = [], []
    for i, (src, dst) in enumerate(((k_in, kvs.at[c, 0]), (v_in, kvs.at[c, 1]))):
        rem.append(rcopy(src.at[1 - y], dst.at[my_rows], in_snd.at[i], in_rcv.at[i], peer))
        loc.append(pltpu.make_async_copy(src.at[y], dst.at[my_rows], in_loc.at[i]))
    for h in range(heads):
        rem.append(rcopy(q_in.at[1 - y, h], qs.at[h, my_rows], in_snd.at[2 + h], in_rcv.at[2 + h], peer))
    rem.append(rcopy(do_in.at[1 - y], dos.at[:, my_rows], in_snd.at[2 + heads], in_rcv.at[2 + heads], peer))
    loc.append(pltpu.make_async_copy(q_in.at[y], qs.at[:, my_rows], in_loc.at[2]))
    loc.append(pltpu.make_async_copy(do_in.at[y], dos.at[:, my_rows], in_loc.at[3]))
    for cp in rem:
        cp.start()
    for cp in loc:
        cp.start()
    for i in (0, 1):
        loc[i].wait()
        rem[i].wait_recv()

    def kv_z(t):
        return rcopy(kvs.at[c], kvs.at[c], kv_zs.at[t], kv_rcv.at[c], {"ctxo": t})

    def kv_fwd(p):
        b = 2 * p + m
        return rcopy(kvs.at[b], kvs.at[b], kv_fs.at[p], kv_rcv.at[b], sib)

    def kv_wait(b):
        rcopy(kvs.at[b], kvs.at[b], kv_fs.at[0], kv_rcv.at[b], sib).wait_recv()

    for t in range(nz - 1, 0, -1):
        @pl.when(z < t)
        def _():
            kv_z(t).start()

    kv_fwd(z).start()

    def prep_kv(b):
        kT[b] = kvs[b, 0].T
        vT[b] = kvs[b, 1].T

    prep_kv(c)
    loc[2].wait()

    def prep_q(h):
        rcopy(q_in.at[1 - y, h], qs.at[h, my_rows], in_snd.at[2 + h], in_rcv.at[2 + h], peer).wait_recv()
        qT[h] = qs[h].T

    def tri():
        r = lax.broadcasted_iota(jnp.int32, (tile, tile), 0)
        s = lax.broadcasted_iota(jnp.int32, (tile, tile), 1)
        return s >= r

    def span(t, kind):
        if kind == DIAG:
            return (t + 1) * tile
        return half if kind == SIB and (t + 1) * tile <= half else chip_len

    def cols(t):
        return slice(t * tile, (t + 1) * tile)

    def masked(s, t, kind, fill):
        nk = span(t, kind)
        if kind == DIAG:
            low = jnp.where(tri(), s[nk - tile:], fill)
            return jnp.concatenate([s[:nk - tile], low], axis=0) if nk > tile else low
        if kind == SIB:
            row = lax.broadcasted_iota(jnp.int32, (1, tile), 1) + t * tile
            seen = m * half + jnp.where(row >= half, half, 0)
            return jnp.where(lax.broadcasted_iota(jnp.int32, s.shape, 0) < seen, s, fill)
        return s

    def put_scores(t, kind, s):
        s = masked(s, t, kind, -jnp.inf)
        sb[:span(t, kind), cols(t)] = s
        mbr[:, cols(t)] = jnp.max(s, axis=0, keepdims=True)

    def scores(b, h, t, kind):
        return dot(kvs[b, 0, :span(t, kind), :], qT[h, :, cols(t)])

    def fwd_step(b, h, kind, bn, hn, kind_n):
        for t in range(n_tiles):
            sl = cols(t)
            nk = span(t, kind)
            top = mbr[:, sl]
            if kind != DIAG:
                old = mr[h, :, sl]
                top = jnp.maximum(old, top)
                fade = jnp.exp2((old - top) * c2)
            s = sb[:nk, sl]
            sn = scores(bn, hn, t, kind_n)
            p = jnp.exp2((s - top) * c2)
            tot = jnp.sum(p, axis=0, keepdims=True)
            o = dot(vT[b, :, :nk], p.astype(BF))
            put_scores(t, kind_n, sn)
            if kind == DIAG:
                lr[h, :, sl] = tot
                oT[h, :, sl] = o
            else:
                lr[h, :, sl] = lr[h, :, sl] * fade + tot
                oT[h, :, sl] = oT[h, :, sl] * fade + o
            mr[h, :, sl] = top

    def fwd_block(i):
        b = 2 * (z - 1 - i // 2) + jnp.where(lax.rem(i, 2) == 0, m, 1 - m)
        return jnp.where(i >= 2 * z, c, b)

    def arrive(i):
        b = fwd_block(i)

        @pl.when(i < 2 * z)
        def _():
            kv_wait(b)

            @pl.when(lax.rem(i, 2) == 0)
            def _():
                kv_fwd(z - 1 - i // 2).start()

            prep_kv(b)

    def start_scores(b, h, kind):
        for t in range(n_tiles):
            put_scores(t, kind, scores(b, h, t, kind))

    sb_blk = 2 * z + 1 - m
    prep_q(0)
    start_scores(c, 0, DIAG)
    kv_wait(sb_blk)
    prep_kv(sb_blk)

    def fwd_plane(h, _):
        hn = jnp.minimum(h + 1, heads - 1)

        @pl.when(h + 1 < heads)
        def _():
            prep_q(h + 1)

        fwd_step(c, h, DIAG, sb_blk, h, SIB)
        fwd_step(sb_blk, h, SIB, c, hn, DIAG)
        return 0

    lax.fori_loop(0, heads, fwd_plane, 0)
    arrive(0)
    start_scores(fwd_block(0), 0, FULL)

    def fwd_full(n, _):
        i = n // heads
        h = n - i * heads
        last = h == heads - 1

        @pl.when(last)
        def _():
            arrive(i + 1)

        fwd_step(fwd_block(i), h, FULL, fwd_block(jnp.where(last, i + 1, i)), jnp.where(last, 0, h + 1), FULL)
        return 0

    lax.fori_loop(0, 2 * z * heads, fwd_full, 0)

    loc[3].wait()
    rem[-1].wait_recv()

    def fwd_end(h, _):
        doT[h] = dos[h].T
        l = lr[h]
        o = oT[h] / l
        mr[h] = mr[h] * c2 + jnp.log2(l)
        dr[h] = jnp.sum(o * dos[h].T.astype(F32), axis=0, keepdims=True)
        os[h] = o.T.astype(BF)
        dqT[h] = jnp.zeros_like(o)
        return 0

    lax.fori_loop(0, heads, fwd_end, 0)

    def bwd_step(b, h, kind):
        for t in range(n_tiles):
            sl = cols(t)
            nk = span(t, kind)
            s = dot(kvs[b, 0, :nk, :], qT[h, :, sl])
            dp = dot(kvs[b, 1, :nk, :], doT[h, :, sl])
            p = masked(jnp.exp2(s * c2 - mr[h, :, sl]), t, kind, 0.0)
            ds = (p * (dp - dr[h, :, sl])).astype(BF)
            dkv[b, 1, :nk, :] += dot(p.astype(BF), dos[h, sl, :])
            dkv[b, 0, :nk, :] += dot(ds, qs[h, sl, :])
            dqT[h, :, sl] += dot(kT[b, :, :nk], ds)

    def o_copies():
        return (pltpu.make_async_copy(os.at[:, my_rows], o_out.at[y], o_loc),
                rcopy(os.at[:, peer_rows], o_out.at[y], o_snd, o_rcv, peer))

    def bwd_block(i):
        return i + jnp.where(m == 0, 1 - 2 * lax.rem(i, 2), 0)

    def y_send(p):
        return rcopy(dkv.at[2 * p + 1 - m], ybuf.at[p], y_snd.at[p], y_rcv.at[p], sib)

    def z_send(p):
        return rcopy(dkv.at[2 * p + m], zbuf.at[z], z_snd.at[p], z_rcv.at[z], {"ctxo": p})

    def y_wait(p):
        rcopy(dkv.at[0], ybuf.at[p], y_snd.at[p], y_rcv.at[p], sib).wait_recv()

    def bwd_full(i, _):
        b = bwd_block(i)
        dkv[b] = jnp.zeros_like(dkv[b])

        def one(h, _):
            bwd_step(b, h, FULL)
            return 0

        lax.fori_loop(0, heads, one, 0)
        p = i // 2

        @pl.when(lax.rem(i, 2) == 0)
        def _():
            y_send(p).start()

        @pl.when(lax.rem(i, 2) == 1)
        def _():
            y_wait(p)
            dkv[b] = dkv[b] + ybuf[p]
            z_send(p).start()

        return 0

    for cp in o_copies():
        cp.start()
    lax.fori_loop(0, 2 * z, bwd_full, 0)

    dkv[c] = jnp.zeros_like(dkv[c])
    dkv[sb_blk] = jnp.zeros_like(dkv[sb_blk])

    def dq_copies(h):
        return (pltpu.make_async_copy(dqs.at[h, my_rows], dq_out.at[y, h], dq_loc.at[h]),
                rcopy(dqs.at[h, peer_rows], dq_out.at[y, h], dq_snd.at[h], dq_rcv.at[h], peer))

    def bwd_diag(h, _):
        bwd_step(sb_blk, h, SIB)
        bwd_step(c, h, DIAG)
        dqs[h] = (dqT[h] * scale).T.astype(BF)

        @pl.when(h > 0)
        def _():
            for cp in dq_copies(h - 1):
                cp.start()

        return 0

    lax.fori_loop(0, heads, bwd_diag, 0)
    for cp in dq_copies(heads - 1):
        cp.start()

    y_send(z).start()

    for t in range(nz - 1, 0, -1):
        @pl.when(z < t)
        def _():
            rcopy(dkv.at[0], zbuf.at[t], z_snd.at[0], z_rcv.at[t], {"ctxo": t}).wait_recv()
            dkv[c] = dkv[c] + zbuf[t]

    y_wait(z)
    dkv[c] = dkv[c] + ybuf[z]

    gs[0] = (dkv[c, 0] * scale).astype(BF)
    gs[1] = dkv[c, 1].astype(BF)
    outs = (dk_out, dv_out)
    g_copies = []
    for i in (0, 1):
        g_copies.append((pltpu.make_async_copy(gs.at[i, my_rows], outs[i].at[y], g_loc.at[i]),
                         rcopy(gs.at[i, peer_rows], outs[i].at[y], g_snd.at[i], g_rcv.at[i], peer)))
        for cp in g_copies[-1]:
            cp.start()

    for cp in rem:
        cp.wait_send()
    for t in range(1, nz):
        @pl.when(z < t)
        def _():
            kv_z(t).wait_send()
    for p in range(nz):
        @pl.when(p <= z)
        def _():
            kv_fwd(p).wait_send()
            y_send(p).wait_send()

        @pl.when(p < z)
        def _():
            z_send(p).wait_send()
    a, b = o_copies()
    a.wait()
    b.wait()
    for h in range(heads):
        a, b = dq_copies(h)
        a.wait()
        b.wait()
    for a, b in g_copies:
        a.wait()
        b.wait()


def solution(mesh):
    nz = mesh.shape["ctxo"]
    spec = P("data", ("ctxo", "ctx"), None, None)

    def local(q, k, v, do):
        rows, half, heads, dim = q.shape
        n = 2 * half
        nb = 2 * nz
        q, do = jnp.swapaxes(q, 1, 2), jnp.swapaxes(do, 1, 2)
        k, v = k[:, :, 0], v[:, :, 0]
        hbm = pl.BlockSpec(memory_space=pl.ANY)
        dma = pltpu.SemaphoreType.DMA
        S = jax.ShapeDtypeStruct
        V = pltpu.VMEM
        o, dq, dk, dv = pl.pallas_call(
            functools.partial(kernel, nz),
            out_shape=[S(q.shape, BF), S(q.shape, BF), S(k.shape, BF), S(k.shape, BF)],
            in_specs=[hbm] * 4,
            out_specs=[hbm] * 4,
            scratch_shapes=[
                V((heads, n, dim), BF), V((heads, n, dim), BF), V((heads, dim, n), BF), V((heads, dim, n), BF),
                V((nb, 2, n, dim), BF), V((nb, dim, n), BF), V((nb, dim, n), BF),
                V((heads, dim, n), F32), V((heads, dim, n), F32),
                V((heads, 1, n), F32), V((heads, 1, n), F32), V((heads, 1, n), F32),
                V((n, n), F32), V((1, n), F32),
                V((nb, 2, n, dim), F32), V((nz, 2, n, dim), F32), V((nz, 2, n, dim), F32),
                V((heads, n, dim), BF), V((heads, n, dim), BF), V((2, n, dim), BF),
                dma((4,)), dma((3 + heads,)), dma((3 + heads,)), dma((nz,)), dma((nz,)), dma((nb,)),
                dma((nz,)), dma((nz,)), dma((nz,)), dma((nz,)),
                dma, dma, dma, dma((2,)), dma((2,)), dma((2,)), dma((heads,)), dma((heads,)), dma((heads,)),
            ],
            compiler_params=pltpu.CompilerParams(collective_id=0, has_side_effects=True, vmem_limit_bytes=62 * 1024 * 1024),
            name="attn",
        )(q, do, k, v)
        return jnp.swapaxes(o, 1, 2), jnp.swapaxes(dq, 1, 2), dk[:, :, None], dv[:, :, None]

    return jax.shard_map(local, mesh=mesh, in_specs=(spec,) * 4, out_specs=(spec,) * 4, check_vma=False)
```

```python
import functools
import math

import jax
import jax.numpy as jnp
from jax import lax
from jax.experimental import pallas as pl
from jax.experimental.pallas import tpu as pltpu
from jax.sharding import PartitionSpec as P

MESH = pl.DeviceIdType.MESH
BF = jnp.bfloat16
F32 = jnp.float32
DIAG, SIB, FULL = 0, 1, 2
GIVE3, GIVE2 = 2, 0
EXTRA = max(GIVE3, GIVE2)


def dot(a, b):
    return jnp.dot(a, b, preferred_element_type=F32)


def either(*conds):
    return functools.reduce(jnp.logical_or, conds)


def both(*conds):
    return functools.reduce(jnp.logical_and, conds)


def loop(n, body):
    def step(i, carry):
        body(i)
        return carry

    lax.fori_loop(0, n, step, 0)


def kernel(heads, q_in, do_in, k_in, v_in, o_out, dq_out, dk_out, dv_out,
           qs, dos, qT, doT, kvs, kT, vT, oT, dqT, mr, lr, dr, sb, mbr, dkv, ybuf, zbuf, cbuf, os, dqs, gs,
           kv_loc, kv_snd, kv_xrc, qd_loc, q_snd, q_rcv, d_snd, d_rcv, hq_snd, hq_rcv, hd_snd, hd_rcv,
           kv_zs, kv_fs, kv_rcv, y_snd, y_rcv, z_snd, z_rcv, c_rcv,
           o_loc, o_snd, o_rcv, dq_loc, dq_snd, dq_rcv, ho_snd, ho_rcv, hg_snd, hg_rcv, g_loc, g_snd, g_rcv):
    _, chip_len, dim = qs.shape
    nz = 4
    half = chip_len // 2
    tile = min(256, chip_len)
    n_tiles = chip_len // tile
    scale = 1.0 / math.sqrt(dim)
    c2 = scale * math.log2(math.e)

    z = lax.axis_index("ctxo")
    x = lax.axis_index("ctx")
    m = lax.rem(x, 2)
    y = x // 2
    zs = nz - 1 - z
    give = jnp.where(z == 3, GIVE3, jnp.where(z == 2, GIVE2, 0))
    take = jnp.where(z == 0, GIVE3, jnp.where(z == 1, GIVE2, 0))
    n_own = heads - give
    helps = take > 0
    c = 2 * z + m
    peer = {"ctx": 2 * (1 - y) + m}
    sib = {"ctx": 2 * y + 1 - m}
    mates = ({"ctxo": zs}, {"ctxo": zs, "ctx": 2 * (1 - y) + m})
    my_rows = pl.ds(pl.multiple_of(y * half, half), half)
    peer_rows = pl.ds(pl.multiple_of((1 - y) * half, half), half)
    batch = (y, 1 - y)
    rows = (my_rows, peer_rows)

    def rcopy(src, dst, ss, rs, dev):
        return pltpu.make_async_remote_copy(src_ref=src, dst_ref=dst, send_sem=ss, recv_sem=rs, device_id=dev, device_id_type=MESH)

    bar = pltpu.get_barrier_semaphore()
    for dev in (peer, sib, mates[1]) + tuple({"ctxo": lax.rem(z + d, nz)} for d in range(1, nz)):
        pl.semaphore_signal(bar, inc=1, device_id=dev, device_id_type=MESH)
    pl.semaphore_wait(bar, nz + 2)

    def kv_swap(i):
        src = (k_in, v_in)[i]
        return (rcopy(src.at[1 - y], kvs.at[c, i, my_rows], kv_snd.at[i], kv_xrc.at[i], peer),
                pltpu.make_async_copy(src.at[y], kvs.at[c, i, my_rows], kv_loc.at[i]))

    def q_swap(h):
        return rcopy(q_in.at[1 - y, h], qs.at[h, my_rows], q_snd.at[h], q_rcv.at[h], peer)

    def d_swap(h):
        return rcopy(do_in.at[1 - y, h], dos.at[h, my_rows], d_snd.at[h], d_rcv.at[h], peer)

    def q_give(j, r):
        return rcopy(q_in.at[batch[r], jnp.minimum(heads - give + j, heads - 1)], qs.at[heads + j, my_rows], hq_snd.at[j, r], hq_rcv.at[j, r], mates[r])

    def d_give(j, r):
        return rcopy(do_in.at[batch[r], jnp.minimum(heads - give + j, heads - 1)], dos.at[heads + j, my_rows], hd_snd.at[j, r], hd_rcv.at[j, r], mates[r])

    for i in (0, 1):
        for cp in kv_swap(i):
            cp.start()
    loop(n_own, lambda h: q_swap(h).start())
    q_loc = (pltpu.make_async_copy(q_in.at[y], qs.at[:heads, my_rows], qd_loc.at[0]),
             pltpu.make_async_copy(do_in.at[y], dos.at[:heads, my_rows], qd_loc.at[1]))
    for cp in q_loc:
        cp.start()
    dkv[...] = jnp.zeros_like(dkv)
    for i in (0, 1):
        swap, local = kv_swap(i)
        local.wait()
        swap.wait_recv()

    def kv_z(t):
        return rcopy(kvs.at[c], kvs.at[c], kv_zs.at[t], kv_rcv.at[c], {"ctxo": t})

    def kv_goes(t):
        up = z < t
        if t == 0:
            return z > 0 if GIVE3 else z < 0
        if t == 1 and GIVE2:
            return either(up, z == 2)
        return up

    def kv_fwd(p):
        b = 2 * p + m
        return rcopy(kvs.at[b], kvs.at[b], kv_fs.at[p], kv_rcv.at[b], sib)

    def kv_wait(b):
        rcopy(kvs.at[b], kvs.at[b], kv_fs.at[0], kv_rcv.at[b], sib).wait_recv()

    kv_fwd(z).start()
    for t in range(nz - 1, -1, -1):
        @pl.when(kv_goes(t))
        def _():
            kv_z(t).start()

    def give_all(j):
        for r in (0, 1):
            q_give(j, r).start()

    def give_all_d(j):
        for r in (0, 1):
            d_give(j, r).start()

    loop(give, give_all)
    loop(n_own, lambda h: d_swap(h).start())
    loop(give, give_all_d)

    def prep_kv(b):
        kT[b] = kvs[b, 0].T
        vT[b] = kvs[b, 1].T

    prep_kv(c)
    q_loc[0].wait()

    def prep_q(h):
        @pl.when(h < heads)
        def _():
            q_swap(jnp.minimum(h, heads - 1)).wait_recv()

        if EXTRA:
            @pl.when(h >= heads)
            def _():
                for r in (0, 1):
                    q_give(jnp.maximum(h - heads, 0), r).wait_recv()

        qT[h] = qs[h].T

    def tri():
        r = lax.broadcasted_iota(jnp.int32, (tile, tile), 0)
        s = lax.broadcasted_iota(jnp.int32, (tile, tile), 1)
        return s >= r

    def span(t, kind):
        if kind == DIAG:
            return (t + 1) * tile
        return half if kind == SIB and (t + 1) * tile <= half else chip_len

    def cols(t):
        return slice(t * tile, (t + 1) * tile)

    def masked(s, t, kind, fill):
        nk = span(t, kind)
        if kind == DIAG:
            low = jnp.where(tri(), s[nk - tile:], fill)
            return jnp.concatenate([s[:nk - tile], low], axis=0) if nk > tile else low
        if kind == SIB:
            row = lax.broadcasted_iota(jnp.int32, (1, tile), 1) + t * tile
            seen = m * half + jnp.where(row >= half, half, 0)
            return jnp.where(lax.broadcasted_iota(jnp.int32, s.shape, 0) < seen, s, fill)
        return s

    def put_scores(t, kind, s):
        s = masked(s, t, kind, -jnp.inf)
        sb[:span(t, kind), cols(t)] = s
        mbr[:, cols(t)] = jnp.max(s, axis=0, keepdims=True)

    def scores(b, h, t, kind):
        return dot(kvs[b, 0, :span(t, kind), :], qT[h, :, cols(t)])

    def start_scores(b, h, kind):
        for t in range(n_tiles):
            put_scores(t, kind, scores(b, h, t, kind))

    def fwd_step(b, h, kind, bn, hn, kind_n):
        for t in range(n_tiles):
            sl = cols(t)
            nk = span(t, kind)
            top = mbr[:, sl]
            if kind != DIAG:
                old = mr[h, :, sl]
                top = jnp.maximum(old, top)
                fade = jnp.exp2((old - top) * c2)
            s = sb[:nk, sl]
            sn = scores(bn, hn, t, kind_n)
            p = jnp.exp2((s - top) * c2)
            tot = jnp.sum(p, axis=0, keepdims=True)
            o = dot(vT[b, :, :nk], p.astype(BF))
            put_scores(t, kind_n, sn)
            if kind == DIAG:
                lr[h, :, sl] = tot
                oT[h, :, sl] = o
            else:
                lr[h, :, sl] = lr[h, :, sl] * fade + tot
                oT[h, :, sl] = oT[h, :, sl] * fade + o
            mr[h, :, sl] = top

    def fwd_part(part):
        own = part == 0
        zq = jnp.where(own, z, zs)
        h0 = jnp.where(own, 0, heads)
        nh = jnp.where(own, n_own, take)
        cb = 2 * zq + m
        sbk = 2 * zq + 1 - m

        def fwd_block(i):
            b = 2 * (zq - 1 - i // 2) + jnp.where(lax.rem(i, 2) == 0, m, 1 - m)
            return jnp.where(i >= 2 * zq, cb, b)

        def arrive(i):
            b = fwd_block(i)
            p = zq - 1 - i // 2

            @pl.when(both(i < 2 * zq, either(own, p > z)))
            def _():
                kv_wait(b)

                @pl.when(lax.rem(i, 2) == 0)
                def _():
                    kv_fwd(jnp.maximum(p, 0)).start()

                prep_kv(b)

        def plane(n):
            h = h0 + n

            @pl.when(n + 1 < nh)
            def _():
                prep_q(h + 1)

            fwd_step(cb, h, DIAG, sbk, h, SIB)
            fwd_step(sbk, h, SIB, cb, h0 + jnp.minimum(n + 1, nh - 1), DIAG)

        def full(n):
            i = n // nh
            k = n - i * nh
            last = k == nh - 1

            @pl.when(last)
            def _():
                arrive(i + 1)

            fwd_step(fwd_block(i), h0 + k, FULL, fwd_block(jnp.where(last, i + 1, i)), h0 + jnp.where(last, 0, k + 1), FULL)

        @pl.when(nh > 0)
        def _():
            @pl.when(jnp.logical_not(own))
            def _():
                kv_wait(cb)
                kv_fwd(zq).start()
                prep_kv(cb)

            prep_q(h0)
            start_scores(cb, h0, DIAG)
            kv_wait(sbk)
            prep_kv(sbk)
            loop(nh, plane)

            @pl.when(zq > 0)
            def _():
                arrive(0)
                start_scores(fwd_block(0), h0, FULL)
                loop(2 * zq * nh, full)

    loop(2 if EXTRA else 1, fwd_part)

    q_loc[1].wait()

    def slot(n):
        return jnp.where(n < n_own, n, n - n_own + heads)

    def fwd_end(n):
        h = slot(n)

        @pl.when(h < heads)
        def _():
            d_swap(jnp.minimum(h, heads - 1)).wait_recv()

        if EXTRA:
            @pl.when(h >= heads)
            def _():
                for r in (0, 1):
                    d_give(jnp.maximum(h - heads, 0), r).wait_recv()

        d = dos[h].T
        doT[h] = d
        l = lr[h]
        o = oT[h] / l
        mr[h] = mr[h] * c2 + jnp.log2(l)
        dr[h] = jnp.sum(o * d.astype(F32), axis=0, keepdims=True)
        os[h] = o.T.astype(BF)
        dqT[h] = jnp.zeros_like(o)

    loop(n_own + take, fwd_end)

    def res_copies(src, dst, loc, snd, rcv, h):
        return (pltpu.make_async_copy(src.at[h, my_rows], dst.at[y, h], loc.at[h]),
                rcopy(src.at[h, peer_rows], dst.at[y, h], snd.at[h], rcv.at[h], peer))

    def o_copies(h):
        return res_copies(os, o_out, o_loc, o_snd, o_rcv, h)

    def dq_copies(h):
        return res_copies(dqs, dq_out, dq_loc, dq_snd, dq_rcv, h)

    def back(src, dst, snd, rcv, j, r, n):
        return rcopy(src.at[heads + j, rows[r]], dst.at[y, heads - n + j], snd.at[j, r], rcv.at[j, r], mates[r])

    def start_both(pair):
        for cp in pair:
            cp.start()

    loop(n_own, lambda h: start_both(o_copies(h)))
    loop(take, lambda j: start_both(back(os, o_out, ho_snd, ho_rcv, j, r, take) for r in (0, 1)))

    def bwd_step(b, h, kind):
        for t in range(n_tiles):
            sl = cols(t)
            nk = span(t, kind)
            s = dot(kvs[b, 0, :nk, :], qT[h, :, sl])
            dp = dot(kvs[b, 1, :nk, :], doT[h, :, sl])
            p = masked(jnp.exp2(s * c2 - mr[h, :, sl]), t, kind, 0.0)
            ds = (p * (dp - dr[h, :, sl])).astype(BF)
            dkv[b, 1, :nk, :] += dot(p.astype(BF), dos[h, sl, :])
            dkv[b, 0, :nk, :] += dot(ds, qs[h, sl, :])
            dqT[h, :, sl] += dot(kT[b, :, :nk], ds)

    def y_send(p):
        return rcopy(dkv.at[2 * p + 1 - m], ybuf.at[p], y_snd.at[p], y_rcv.at[p], sib)

    def y_add(p):
        rcopy(dkv.at[0], ybuf.at[p], y_snd.at[p], y_rcv.at[p], sib).wait_recv()
        dkv[2 * p + m] = dkv[2 * p + m] + ybuf[p]

    def z_send(p):
        return rcopy(dkv.at[2 * p + m], zbuf.at[z], z_snd.at[p], z_rcv.at[z], {"ctxo": p})

    def c_send(p):
        return rcopy(dkv.at[2 * p + m], cbuf.at[p], z_snd.at[p], c_rcv.at[p], {"ctxo": 2})

    def leave(p):
        @pl.when(both(z == 3, p < 2))
        def _():
            c_send(jnp.minimum(p, 1)).start()

        @pl.when(either(both(z == 3, p == 2), z < 2))
        def _():
            z_send(p).start()

    def chain(p):
        rcopy(dkv.at[0], cbuf.at[p], z_snd.at[p], c_rcv.at[p], {"ctxo": 2}).wait_recv()
        dkv[2 * p + m] = dkv[2 * p + m] + cbuf[p]
        z_send(p).start()

    def finish_dq(h):
        dqs[h] = (dqT[h] * scale).T.astype(BF)

    n_planes = jnp.where(helps, zs, z)

    def bwd_full(i):
        k = i // 2
        p = jnp.where(helps, n_planes - 1 - k, k)
        first = lax.rem(i, 2) == 0
        b = 2 * p + jnp.where(first, 1 - m, m)
        na = jnp.where(p < z, n_own, 0)
        nb = take

        def one(n):
            bwd_step(b, jnp.where(n < na, n, n - na + heads), FULL)

        loop(na + nb, one)

        @pl.when(both(first, p != z))
        def _():
            y_send(p).start()

        if EXTRA:
            @pl.when(both(helps, i == 0))
            def _():
                y_add(zs)
                leave(zs)

        @pl.when(both(jnp.logical_not(first), p != z))
        def _():
            y_add(p)
            leave(p)

        @pl.when(both(z == 2, i == 3))
        def _():
            chain(0)

    def bwd_part(part):
        own = part == 1
        zq = jnp.where(own, z, zs)
        h0 = jnp.where(own, 0, heads)

        def plane(n):
            h = h0 + n
            bwd_step(2 * zq + 1 - m, h, SIB)
            bwd_step(2 * zq + m, h, DIAG)

            @pl.when(own)
            def _():
                finish_dq(h)

                @pl.when(h > 0)
                def _():
                    start_both(dq_copies(jnp.clip(h - 1, 0, heads - 1)))

                @pl.when(both(z == 2, h == 3))
                def _():
                    chain(1)

        loop(jnp.where(own, n_own, take), plane)

        @pl.when(either(own, helps))
        def _():
            y_send(zq).start()

        @pl.when(jnp.logical_not(own))
        def _():
            loop(2 * n_planes, bwd_full)

            def taken_dq(j):
                finish_dq(heads + j)

            loop(take, taken_dq)
            loop(take, lambda j: start_both(back(dqs, dq_out, hg_snd, hg_rcv, j, r, take) for r in (0, 1)))

    loop(2, bwd_part)
    start_both(dq_copies(n_own - 1))

    def z_comes(t):
        if t == 3:
            return z == 2
        if t == 2:
            return z < 2
        if t == 1:
            return either(z == 0, z == 2) if GIVE2 else z == 0
        return z > 0 if GIVE3 else z < 0

    for t in range(nz):
        @pl.when(z_comes(t))
        def _():
            rcopy(dkv.at[0], zbuf.at[t], z_snd.at[0], z_rcv.at[t], {"ctxo": t}).wait_recv()
            dkv[c] = dkv[c] + zbuf[t]

    y_add(z)
    gs[0] = (dkv[c, 0] * scale).astype(BF)
    gs[1] = dkv[c, 1].astype(BF)
    outs = (dk_out, dv_out)
    g_copies = []
    for i in (0, 1):
        g_copies.append((pltpu.make_async_copy(gs.at[i, my_rows], outs[i].at[y], g_loc.at[i]),
                         rcopy(gs.at[i, peer_rows], outs[i].at[y], g_snd.at[i], g_rcv.at[i], peer)))
        start_both(g_copies[-1])

    for i in (0, 1):
        kv_swap(i)[0].wait_send()

    def own_sent(h):
        q_swap(h).wait_send()
        d_swap(h).wait_send()
        for a, b in (o_copies(h), dq_copies(h)):
            a.wait()
            b.wait()

    loop(n_own, own_sent)

    def given(j):
        for r in (0, 1):
            q_give(j, r).wait_send()
            d_give(j, r).wait_send()
            for dst, snd, rcv in ((o_out, ho_snd, ho_rcv), (dq_out, hg_snd, hg_rcv)):
                rcopy(os.at[0, my_rows], dst.at[batch[r], heads - give + j], snd.at[j, r], rcv.at[j, r], mates[r]).wait_recv()

    def taken(j):
        for r in (0, 1):
            back(os, o_out, ho_snd, ho_rcv, j, r, take).wait_send()
            back(dqs, dq_out, hg_snd, hg_rcv, j, r, take).wait_send()

    if EXTRA:
        loop(give, given)
        loop(take, taken)

    for t in range(nz):
        @pl.when(kv_goes(t))
        def _():
            kv_z(t).wait_send()

    def planes_sent(p):
        kv_fwd(p).wait_send()
        y_send(p).wait_send()

        @pl.when(p != z)
        def _():
            z_send(p).wait_send()

    loop(jnp.where(helps, zs, z) + 1, planes_sent)
    for a, b in g_copies:
        a.wait()
        b.wait()


def solution(mesh):
    nz = mesh.shape["ctxo"]
    spec = P("data", ("ctxo", "ctx"), None, None)

    def local(q, k, v, do):
        rows, half, heads, dim = q.shape
        n = 2 * half
        nb = 2 * nz
        nh = heads + EXTRA
        ex = max(EXTRA, 1)
        q, do = jnp.swapaxes(q, 1, 2), jnp.swapaxes(do, 1, 2)
        k, v = k[:, :, 0], v[:, :, 0]
        hbm = pl.BlockSpec(memory_space=pl.ANY)
        S = jax.ShapeDtypeStruct
        V = pltpu.VMEM

        def dma(*shape):
            return pltpu.SemaphoreType.DMA(shape)

        o, dq, dk, dv = pl.pallas_call(
            functools.partial(kernel, heads),
            out_shape=[S(q.shape, BF), S(q.shape, BF), S(k.shape, BF), S(k.shape, BF)],
            in_specs=[hbm] * 4,
            out_specs=[hbm] * 4,
            scratch_shapes=[
                V((nh, n, dim), BF), V((nh, n, dim), BF), V((nh, dim, n), BF), V((nh, dim, n), BF),
                V((nb, 2, n, dim), BF), V((nb, dim, n), BF), V((nb, dim, n), BF),
                V((nh, dim, n), F32), V((nh, dim, n), F32),
                V((nh, 1, n), F32), V((nh, 1, n), F32), V((nh, 1, n), F32),
                V((n, n), F32), V((1, n), F32),
                V((nb, 2, n, dim), F32), V((nz, 2, n, dim), F32), V((nz, 2, n, dim), F32), V((2, 2, n, dim), F32),
                V((nh, n, dim), BF), V((nh, n, dim), BF), V((2, n, dim), BF),
                dma(2), dma(2), dma(2), dma(2), dma(heads), dma(heads), dma(heads), dma(heads),
                dma(ex, 2), dma(ex, 2), dma(ex, 2), dma(ex, 2),
                dma(nz), dma(nz), dma(nb), dma(nz), dma(nz), dma(nz), dma(nz), dma(2),
                dma(heads), dma(heads), dma(heads), dma(heads), dma(heads), dma(heads),
                dma(ex, 2), dma(ex, 2), dma(ex, 2), dma(ex, 2), dma(2), dma(2), dma(2),
            ],
            compiler_params=pltpu.CompilerParams(collective_id=0, has_side_effects=True, vmem_limit_bytes=62 * 1024 * 1024),
            name="attn",
        )(q, do, k, v)
        return jnp.swapaxes(o, 1, 2), jnp.swapaxes(dq, 1, 2), dk[:, :, None], dv[:, :, None]

    return jax.shard_map(local, mesh=mesh, in_specs=(spec,) * 4, out_specs=(spec,) * 4, check_vma=False)
```

```python
import functools
import math

import jax
import jax.numpy as jnp
from jax import lax
from jax.experimental import pallas as pl
from jax.experimental.pallas import tpu as pltpu
from jax.sharding import PartitionSpec as P

MESH = pl.DeviceIdType.MESH
BF = jnp.bfloat16
F32 = jnp.float32
DIAG, SIB, FULL = 0, 1, 2
GIVE3, GIVE2 = 2, 0
EXTRA = max(GIVE3, GIVE2)


def dot(a, b):
    return jnp.dot(a, b, preferred_element_type=F32)


def either(*conds):
    return functools.reduce(jnp.logical_or, conds)


def both(*conds):
    return functools.reduce(jnp.logical_and, conds)


def loop(n, body):
    def step(i, carry):
        body(i)
        return carry

    lax.fori_loop(0, n, step, 0)


def kernel(heads, q_in, do_in, k_in, v_in, o_out, dq_out, dk_out, dv_out,
           qs, dos, qT, doT, kvs, kT, vT, oT, dqT, mr, lr, dr, sb, mbr, dkv, ybuf, zbuf, cbuf, os, dqs, gs,
           kv_loc, kv_snd, kv_xrc, qd_loc, q_snd, q_rcv, d_snd, d_rcv, hq_snd, hq_rcv, hd_snd, hd_rcv,
           kv_zs, kv_fs, kv_rcv, y_snd, y_rcv, z_snd, z_rcv, c_rcv,
           o_loc, o_snd, o_rcv, dq_loc, dq_snd, dq_rcv, ho_snd, ho_rcv, hg_snd, hg_rcv, g_loc, g_snd, g_rcv):
    _, chip_len, dim = qs.shape
    nz = 4
    half = chip_len // 2
    tile = min(256, chip_len)
    n_tiles = chip_len // tile
    scale = 1.0 / math.sqrt(dim)
    c2 = scale * math.log2(math.e)

    z = lax.axis_index("ctxo")
    x = lax.axis_index("ctx")
    m = lax.rem(x, 2)
    y = x // 2
    zs = nz - 1 - z
    give = jnp.where(z == 3, GIVE3, jnp.where(z == 2, GIVE2, 0))
    take = jnp.where(z == 0, GIVE3, jnp.where(z == 1, GIVE2, 0))
    n_own = heads - give
    helps = take > 0
    c = 2 * z + m
    peer = {"ctx": 2 * (1 - y) + m}
    sib = {"ctx": 2 * y + 1 - m}
    mates = ({"ctxo": zs}, {"ctxo": zs, "ctx": 2 * (1 - y) + m})
    my_rows = pl.ds(pl.multiple_of(y * half, half), half)
    peer_rows = pl.ds(pl.multiple_of((1 - y) * half, half), half)
    batch = (y, 1 - y)
    rows = (my_rows, peer_rows)

    def rcopy(src, dst, ss, rs, dev):
        return pltpu.make_async_remote_copy(src_ref=src, dst_ref=dst, send_sem=ss, recv_sem=rs, device_id=dev, device_id_type=MESH)

    bar = pltpu.get_barrier_semaphore()
    for dev in (peer, sib, mates[1]) + tuple({"ctxo": lax.rem(z + d, nz)} for d in range(1, nz)):
        pl.semaphore_signal(bar, inc=1, device_id=dev, device_id_type=MESH)
    pl.semaphore_wait(bar, nz + 2)

    def kv_swap(i):
        src = (k_in, v_in)[i]
        return (rcopy(src.at[1 - y], kvs.at[c, i, my_rows], kv_snd.at[i], kv_xrc.at[i], peer),
                pltpu.make_async_copy(src.at[y], kvs.at[c, i, my_rows], kv_loc.at[i]))

    def q_swap(h):
        return rcopy(q_in.at[1 - y, h], qs.at[h, my_rows], q_snd.at[h], q_rcv.at[h], peer)

    def d_swap(h):
        return rcopy(do_in.at[1 - y, h], dos.at[h, my_rows], d_snd.at[h], d_rcv.at[h], peer)

    def q_give(j, r):
        return rcopy(q_in.at[batch[r], jnp.minimum(heads - give + j, heads - 1)], qs.at[heads + j, my_rows], hq_snd.at[j, r], hq_rcv.at[j, r], mates[r])

    def d_give(j, r):
        return rcopy(do_in.at[batch[r], jnp.minimum(heads - give + j, heads - 1)], dos.at[heads + j, my_rows], hd_snd.at[j, r], hd_rcv.at[j, r], mates[r])

    for i in (0, 1):
        for cp in kv_swap(i):
            cp.start()
    q_loc = (pltpu.make_async_copy(q_in.at[y], qs.at[:heads, my_rows], qd_loc.at[0]),
             pltpu.make_async_copy(do_in.at[y], dos.at[:heads, my_rows], qd_loc.at[1]))
    for cp in q_loc:
        cp.start()
    dkv[...] = jnp.zeros_like(dkv)
    for i in (0, 1):
        swap, local = kv_swap(i)
        local.wait()
        swap.wait_recv()
    loop(n_own, lambda h: q_swap(h).start())

    def kv_z(t):
        return rcopy(kvs.at[c], kvs.at[c], kv_zs.at[t], kv_rcv.at[c], {"ctxo": t})

    def kv_goes(t):
        up = z < t
        if t == 0:
            return z > 0 if GIVE3 else z < 0
        if t == 1 and GIVE2:
            return either(up, z == 2)
        return up

    def kv_fwd(p):
        b = 2 * p + m
        return rcopy(kvs.at[b], kvs.at[b], kv_fs.at[p], kv_rcv.at[b], sib)

    def kv_wait(b):
        rcopy(kvs.at[b], kvs.at[b], kv_fs.at[0], kv_rcv.at[b], sib).wait_recv()

    kv_fwd(z).start()
    for t in range(nz - 1, -1, -1):
        @pl.when(kv_goes(t))
        def _():
            kv_z(t).start()

    def give_all(j):
        for r in (0, 1):
            q_give(j, r).start()

    def give_all_d(j):
        for r in (0, 1):
            d_give(j, r).start()

    loop(give, give_all)
    loop(n_own, lambda h: d_swap(h).start())
    loop(give, give_all_d)

    def prep_kv(b):
        kT[b] = kvs[b, 0].T
        vT[b] = kvs[b, 1].T

    prep_kv(c)
    q_loc[0].wait()

    def prep_q(h):
        @pl.when(h < heads)
        def _():
            q_swap(jnp.minimum(h, heads - 1)).wait_recv()

        if EXTRA:
            @pl.when(h >= heads)
            def _():
                for r in (0, 1):
                    q_give(jnp.maximum(h - heads, 0), r).wait_recv()

        qT[h] = qs[h].T

    def tri():
        r = lax.broadcasted_iota(jnp.int32, (tile, tile), 0)
        s = lax.broadcasted_iota(jnp.int32, (tile, tile), 1)
        return s >= r

    def span(t, kind):
        if kind == DIAG:
            return (t + 1) * tile
        return half if kind == SIB and (t + 1) * tile <= half else chip_len

    def cols(t):
        return slice(t * tile, (t + 1) * tile)

    def masked(s, t, kind, fill):
        nk = span(t, kind)
        if kind == DIAG:
            low = jnp.where(tri(), s[nk - tile:], fill)
            return jnp.concatenate([s[:nk - tile], low], axis=0) if nk > tile else low
        if kind == SIB:
            row = lax.broadcasted_iota(jnp.int32, (1, tile), 1) + t * tile
            seen = m * half + jnp.where(row >= half, half, 0)
            return jnp.where(lax.broadcasted_iota(jnp.int32, s.shape, 0) < seen, s, fill)
        return s

    def put_scores(t, kind, s):
        s = masked(s, t, kind, -jnp.inf)
        sb[:span(t, kind), cols(t)] = s
        mbr[:, cols(t)] = jnp.max(s, axis=0, keepdims=True)

    def scores(b, h, t, kind):
        return dot(kvs[b, 0, :span(t, kind), :], qT[h, :, cols(t)])

    def start_scores(b, h, kind):
        for t in range(n_tiles):
            put_scores(t, kind, scores(b, h, t, kind))

    def fwd_step(b, h, kind, bn, hn, kind_n):
        for t in range(n_tiles):
            sl = cols(t)
            nk = span(t, kind)
            top = mbr[:, sl]
            if kind != DIAG:
                old = mr[h, :, sl]
                top = jnp.maximum(old, top)
                fade = jnp.exp2((old - top) * c2)
            s = sb[:nk, sl]
            sn = scores(bn, hn, t, kind_n)
            p = jnp.exp2((s - top) * c2)
            tot = jnp.sum(p, axis=0, keepdims=True)
            o = dot(vT[b, :, :nk], p.astype(BF))
            put_scores(t, kind_n, sn)
            if kind == DIAG:
                lr[h, :, sl] = tot
                oT[h, :, sl] = o
            else:
                lr[h, :, sl] = lr[h, :, sl] * fade + tot
                oT[h, :, sl] = oT[h, :, sl] * fade + o
            mr[h, :, sl] = top

    def fwd_part(part):
        own = part == 0
        zq = jnp.where(own, z, zs)
        h0 = jnp.where(own, 0, heads)
        nh = jnp.where(own, n_own, take)
        cb = 2 * zq + m
        sbk = 2 * zq + 1 - m

        def fwd_block(i):
            b = 2 * (zq - 1 - i // 2) + jnp.where(lax.rem(i, 2) == 0, m, 1 - m)
            return jnp.where(i >= 2 * zq, cb, b)

        def arrive(i):
            b = fwd_block(i)
            p = zq - 1 - i // 2

            @pl.when(both(i < 2 * zq, either(own, p > z)))
            def _():
                kv_wait(b)

                @pl.when(lax.rem(i, 2) == 0)
                def _():
                    kv_fwd(jnp.maximum(p, 0)).start()

                prep_kv(b)

        def plane(n):
            h = h0 + n

            @pl.when(n + 1 < nh)
            def _():
                prep_q(h + 1)

            fwd_step(cb, h, DIAG, sbk, h, SIB)
            fwd_step(sbk, h, SIB, cb, h0 + jnp.minimum(n + 1, nh - 1), DIAG)

        def full(n):
            i = n // nh
            k = n - i * nh
            last = k == nh - 1

            @pl.when(last)
            def _():
                arrive(i + 1)

            fwd_step(fwd_block(i), h0 + k, FULL, fwd_block(jnp.where(last, i + 1, i)), h0 + jnp.where(last, 0, k + 1), FULL)

        @pl.when(nh > 0)
        def _():
            @pl.when(jnp.logical_not(own))
            def _():
                kv_wait(cb)
                kv_fwd(zq).start()
                prep_kv(cb)

            prep_q(h0)
            start_scores(cb, h0, DIAG)
            kv_wait(sbk)
            prep_kv(sbk)
            loop(nh, plane)

            @pl.when(zq > 0)
            def _():
                arrive(0)
                start_scores(fwd_block(0), h0, FULL)
                loop(2 * zq * nh, full)

    loop(2 if EXTRA else 1, fwd_part)

    q_loc[1].wait()

    def slot(n):
        return jnp.where(n < n_own, n, n - n_own + heads)

    def fwd_end(n):
        h = slot(n)

        @pl.when(h < heads)
        def _():
            d_swap(jnp.minimum(h, heads - 1)).wait_recv()

        if EXTRA:
            @pl.when(h >= heads)
            def _():
                for r in (0, 1):
                    d_give(jnp.maximum(h - heads, 0), r).wait_recv()

        d = dos[h].T
        doT[h] = d
        l = lr[h]
        o = oT[h] / l
        mr[h] = mr[h] * c2 + jnp.log2(l)
        dr[h] = jnp.sum(o * d.astype(F32), axis=0, keepdims=True)
        os[h] = o.T.astype(BF)
        dqT[h] = jnp.zeros_like(o)

    loop(n_own + take, fwd_end)

    def res_copies(src, dst, loc, snd, rcv, h):
        return (pltpu.make_async_copy(src.at[h, my_rows], dst.at[y, h], loc.at[h]),
                rcopy(src.at[h, peer_rows], dst.at[y, h], snd.at[h], rcv.at[h], peer))

    def o_copies(h):
        return res_copies(os, o_out, o_loc, o_snd, o_rcv, h)

    def dq_copies(h):
        return res_copies(dqs, dq_out, dq_loc, dq_snd, dq_rcv, h)

    def back(src, dst, snd, rcv, j, r, n):
        return rcopy(src.at[heads + j, rows[r]], dst.at[y, heads - n + j], snd.at[j, r], rcv.at[j, r], mates[r])

    def start_both(pair):
        for cp in pair:
            cp.start()

    loop(n_own, lambda h: start_both(o_copies(h)))
    loop(take, lambda j: start_both(back(os, o_out, ho_snd, ho_rcv, j, r, take) for r in (0, 1)))

    def bwd_step(b, h, kind):
        for t in range(n_tiles):
            sl = cols(t)
            nk = span(t, kind)
            s = dot(kvs[b, 0, :nk, :], qT[h, :, sl])
            dp = dot(kvs[b, 1, :nk, :], doT[h, :, sl])
            p = masked(jnp.exp2(s * c2 - mr[h, :, sl]), t, kind, 0.0)
            ds = (p * (dp - dr[h, :, sl])).astype(BF)
            dkv[b, 1, :nk, :] += dot(p.astype(BF), dos[h, sl, :])
            dkv[b, 0, :nk, :] += dot(ds, qs[h, sl, :])
            dqT[h, :, sl] += dot(kT[b, :, :nk], ds)

    def y_send(p):
        return rcopy(dkv.at[2 * p + 1 - m], ybuf.at[p], y_snd.at[p], y_rcv.at[p], sib)

    def y_add(p):
        rcopy(dkv.at[0], ybuf.at[p], y_snd.at[p], y_rcv.at[p], sib).wait_recv()
        dkv[2 * p + m] = dkv[2 * p + m] + ybuf[p]

    def z_send(p):
        return rcopy(dkv.at[2 * p + m], zbuf.at[z], z_snd.at[p], z_rcv.at[z], {"ctxo": p})

    def c_send(p):
        return rcopy(dkv.at[2 * p + m], cbuf.at[p], z_snd.at[p], c_rcv.at[p], {"ctxo": 2})

    def leave(p):
        @pl.when(both(z == 3, p < 2))
        def _():
            c_send(jnp.minimum(p, 1)).start()

        @pl.when(either(both(z == 3, p == 2), z < 2))
        def _():
            z_send(p).start()

    def chain(p):
        rcopy(dkv.at[0], cbuf.at[p], z_snd.at[p], c_rcv.at[p], {"ctxo": 2}).wait_recv()
        dkv[2 * p + m] = dkv[2 * p + m] + cbuf[p]
        z_send(p).start()

    def finish_dq(h):
        dqs[h] = (dqT[h] * scale).T.astype(BF)

    n_planes = jnp.where(helps, zs, z)

    def bwd_full(i):
        k = i // 2
        p = jnp.where(helps, n_planes - 1 - k, k)
        first = lax.rem(i, 2) == 0
        b = 2 * p + jnp.where(first, 1 - m, m)
        na = jnp.where(p < z, n_own, 0)
        nb = take

        def one(n):
            bwd_step(b, jnp.where(n < na, n, n - na + heads), FULL)

        loop(na + nb, one)

        @pl.when(both(first, p != z))
        def _():
            y_send(p).start()

        if EXTRA:
            @pl.when(both(helps, i == 0))
            def _():
                y_add(zs)
                leave(zs)

        @pl.when(both(jnp.logical_not(first), p != z))
        def _():
            y_add(p)
            leave(p)

        @pl.when(both(z == 2, i == 2))
        def _():
            chain(0)

    def bwd_part(part):
        own = part == 1
        zq = jnp.where(own, z, zs)
        h0 = jnp.where(own, 0, heads)

        def plane(n):
            h = h0 + n
            bwd_step(2 * zq + 1 - m, h, SIB)
            bwd_step(2 * zq + m, h, DIAG)

            @pl.when(own)
            def _():
                finish_dq(h)

                @pl.when(h > 0)
                def _():
                    start_both(dq_copies(jnp.clip(h - 1, 0, heads - 1)))

                @pl.when(both(z == 2, h == 1))
                def _():
                    chain(1)

        loop(jnp.where(own, n_own, take), plane)

        @pl.when(either(own, helps))
        def _():
            y_send(zq).start()

        @pl.when(jnp.logical_not(own))
        def _():
            loop(2 * n_planes, bwd_full)

            def taken_dq(j):
                finish_dq(heads + j)

            loop(take, taken_dq)
            loop(take, lambda j: start_both(back(dqs, dq_out, hg_snd, hg_rcv, j, r, take) for r in (0, 1)))

    loop(2, bwd_part)
    start_both(dq_copies(n_own - 1))

    def z_comes(t):
        if t == 3:
            return z == 2
        if t == 2:
            return z < 2
        if t == 1:
            return either(z == 0, z == 2) if GIVE2 else z == 0
        return z > 0 if GIVE3 else z < 0

    for t in range(nz):
        @pl.when(z_comes(t))
        def _():
            rcopy(dkv.at[0], zbuf.at[t], z_snd.at[0], z_rcv.at[t], {"ctxo": t}).wait_recv()
            dkv[c] = dkv[c] + zbuf[t]

    y_add(z)
    gs[0] = (dkv[c, 0] * scale).astype(BF)
    gs[1] = dkv[c, 1].astype(BF)
    outs = (dk_out, dv_out)
    g_copies = []
    for i in (0, 1):
        g_copies.append((pltpu.make_async_copy(gs.at[i, my_rows], outs[i].at[y], g_loc.at[i]),
                         rcopy(gs.at[i, peer_rows], outs[i].at[y], g_snd.at[i], g_rcv.at[i], peer)))
        start_both(g_copies[-1])

    for i in (0, 1):
        kv_swap(i)[0].wait_send()

    def own_sent(h):
        q_swap(h).wait_send()
        d_swap(h).wait_send()
        for a, b in (o_copies(h), dq_copies(h)):
            a.wait()
            b.wait()

    loop(n_own, own_sent)

    def given(j):
        for r in (0, 1):
            q_give(j, r).wait_send()
            d_give(j, r).wait_send()
            for dst, snd, rcv in ((o_out, ho_snd, ho_rcv), (dq_out, hg_snd, hg_rcv)):
                rcopy(os.at[0, my_rows], dst.at[batch[r], heads - give + j], snd.at[j, r], rcv.at[j, r], mates[r]).wait_recv()

    def taken(j):
        for r in (0, 1):
            back(os, o_out, ho_snd, ho_rcv, j, r, take).wait_send()
            back(dqs, dq_out, hg_snd, hg_rcv, j, r, take).wait_send()

    if EXTRA:
        loop(give, given)
        loop(take, taken)

    for t in range(nz):
        @pl.when(kv_goes(t))
        def _():
            kv_z(t).wait_send()

    def planes_sent(p):
        kv_fwd(p).wait_send()
        y_send(p).wait_send()

        @pl.when(p != z)
        def _():
            z_send(p).wait_send()

    loop(jnp.where(helps, zs, z) + 1, planes_sent)
    for a, b in g_copies:
        a.wait()
        b.wait()


def solution(mesh):
    nz = mesh.shape["ctxo"]
    spec = P("data", ("ctxo", "ctx"), None, None)

    def local(q, k, v, do):
        rows, half, heads, dim = q.shape
        n = 2 * half
        nb = 2 * nz
        nh = heads + EXTRA
        ex = max(EXTRA, 1)
        q, do = jnp.swapaxes(q, 1, 2), jnp.swapaxes(do, 1, 2)
        k, v = k[:, :, 0], v[:, :, 0]
        hbm = pl.BlockSpec(memory_space=pl.ANY)
        S = jax.ShapeDtypeStruct
        V = pltpu.VMEM

        def dma(*shape):
            return pltpu.SemaphoreType.DMA(shape)

        o, dq, dk, dv = pl.pallas_call(
            functools.partial(kernel, heads),
            out_shape=[S(q.shape, BF), S(q.shape, BF), S(k.shape, BF), S(k.shape, BF)],
            in_specs=[hbm] * 4,
            out_specs=[hbm] * 4,
            scratch_shapes=[
                V((nh, n, dim), BF), V((nh, n, dim), BF), V((nh, dim, n), BF), V((nh, dim, n), BF),
                V((nb, 2, n, dim), BF), V((nb, dim, n), BF), V((nb, dim, n), BF),
                V((nh, dim, n), F32), V((nh, dim, n), F32),
                V((nh, 1, n), F32), V((nh, 1, n), F32), V((nh, 1, n), F32),
                V((n, n), F32), V((1, n), F32),
                V((nb, 2, n, dim), F32), V((nz, 2, n, dim), F32), V((nz, 2, n, dim), F32), V((2, 2, n, dim), F32),
                V((nh, n, dim), BF), V((nh, n, dim), BF), V((2, n, dim), BF),
                dma(2), dma(2), dma(2), dma(2), dma(heads), dma(heads), dma(heads), dma(heads),
                dma(ex, 2), dma(ex, 2), dma(ex, 2), dma(ex, 2),
                dma(nz), dma(nz), dma(nb), dma(nz), dma(nz), dma(nz), dma(nz), dma(2),
                dma(heads), dma(heads), dma(heads), dma(heads), dma(heads), dma(heads),
                dma(ex, 2), dma(ex, 2), dma(ex, 2), dma(ex, 2), dma(2), dma(2), dma(2),
            ],
            compiler_params=pltpu.CompilerParams(collective_id=0, has_side_effects=True, vmem_limit_bytes=62 * 1024 * 1024),
            name="attn",
        )(q, do, k, v)
        return jnp.swapaxes(o, 1, 2), jnp.swapaxes(dq, 1, 2), dk[:, :, None], dv[:, :, None]

    return jax.shard_map(local, mesh=mesh, in_specs=(spec,) * 4, out_specs=(spec,) * 4, check_vma=False)
```

```python
import functools
import math

import jax
import jax.numpy as jnp
from jax import lax
from jax.experimental import pallas as pl
from jax.experimental.pallas import tpu as pltpu
from jax.sharding import PartitionSpec as P

MESH = pl.DeviceIdType.MESH
BF = jnp.bfloat16
F32 = jnp.float32
DIAG, SIB, FULL = 0, 1, 2
GIVE3, GIVE2 = 2, 0
EXTRA = max(GIVE3, GIVE2)
RELAY1, RELAY2 = 3, 4


def dot(a, b):
    return jnp.dot(a, b, preferred_element_type=F32)


def either(*conds):
    return functools.reduce(jnp.logical_or, conds)


def both(*conds):
    return functools.reduce(jnp.logical_and, conds)


def loop(n, body):
    def step(i, carry):
        body(i)
        return carry

    lax.fori_loop(0, n, step, 0)


def kernel(heads, q_in, do_in, k_in, v_in, o_out, dq_out, dk_out, dv_out,
           qs, dos, qT, doT, kvs, kT, vT, oT, dqT, mr, lr, dr, sb, mbr, dkv, ybuf, zbuf, cbuf, os, dqs, gs,
           kv_loc, kv_snd, kv_xrc, qd_loc, q_snd, q_rcv, d_snd, d_rcv, hq_snd, hq_rcv, hd_snd, hd_rcv,
           kv_us, kv_ds, kv_fs, kv_rcv, y_snd, y_rcv, z_snd, z_rcv, c_rcv,
           o_loc, o_snd, o_rcv, dq_loc, dq_snd, dq_rcv, ho_snd, ho_rcv, hg_snd, hg_rcv, g_loc, g_snd, g_rcv):
    _, chip_len, dim = qs.shape
    nz = 4
    half = chip_len // 2
    tile = min(256, chip_len)
    n_tiles = chip_len // tile
    scale = 1.0 / math.sqrt(dim)
    c2 = scale * math.log2(math.e)

    z = lax.axis_index("ctxo")
    x = lax.axis_index("ctx")
    m = lax.rem(x, 2)
    y = x // 2
    zs = nz - 1 - z
    give = jnp.where(z == 3, GIVE3, jnp.where(z == 2, GIVE2, 0))
    take = jnp.where(z == 0, GIVE3, jnp.where(z == 1, GIVE2, 0))
    n_own = heads - give
    helps = take > 0
    c = 2 * z + m
    peer = {"ctx": 2 * (1 - y) + m}
    sib = {"ctx": 2 * y + 1 - m}
    mates = ({"ctxo": zs}, {"ctxo": zs, "ctx": 2 * (1 - y) + m})
    my_rows = pl.ds(pl.multiple_of(y * half, half), half)
    peer_rows = pl.ds(pl.multiple_of((1 - y) * half, half), half)
    batch = (y, 1 - y)
    rows = (my_rows, peer_rows)

    def rcopy(src, dst, ss, rs, dev):
        return pltpu.make_async_remote_copy(src_ref=src, dst_ref=dst, send_sem=ss, recv_sem=rs, device_id=dev, device_id_type=MESH)

    bar = pltpu.get_barrier_semaphore()
    for dev in (peer, sib, mates[1]) + tuple({"ctxo": lax.rem(z + d, nz)} for d in range(1, nz)):
        pl.semaphore_signal(bar, inc=1, device_id=dev, device_id_type=MESH)
    pl.semaphore_wait(bar, nz + 2)

    def kv_swap(i):
        src = (k_in, v_in)[i]
        return (rcopy(src.at[1 - y], kvs.at[c, i, my_rows], kv_snd.at[i], kv_xrc.at[i], peer),
                pltpu.make_async_copy(src.at[y], kvs.at[c, i, my_rows], kv_loc.at[i]))

    def q_swap(h):
        return rcopy(q_in.at[1 - y, h], qs.at[h, my_rows], q_snd.at[h], q_rcv.at[h], peer)

    def d_swap(h):
        return rcopy(do_in.at[1 - y, h], dos.at[h, my_rows], d_snd.at[h], d_rcv.at[h], peer)

    def q_give(j, r):
        return rcopy(q_in.at[batch[r], jnp.minimum(heads - give + j, heads - 1)], qs.at[heads + j, my_rows], hq_snd.at[j, r], hq_rcv.at[j, r], mates[r])

    def d_give(j, r):
        return rcopy(do_in.at[batch[r], jnp.minimum(heads - give + j, heads - 1)], dos.at[heads + j, my_rows], hd_snd.at[j, r], hd_rcv.at[j, r], mates[r])

    for i in (0, 1):
        for cp in kv_swap(i):
            cp.start()
    q_loc = (pltpu.make_async_copy(q_in.at[y], qs.at[:heads, my_rows], qd_loc.at[0]),
             pltpu.make_async_copy(do_in.at[y], dos.at[:heads, my_rows], qd_loc.at[1]))
    for cp in q_loc:
        cp.start()
    dkv[...] = jnp.zeros_like(dkv)
    for i in (0, 1):
        swap, local = kv_swap(i)
        local.wait()
        swap.wait_recv()
    for h in (0, 1):
        q_swap(h).start()

    def kv_up(p):
        b = 2 * p + m
        return rcopy(kvs.at[b], kvs.at[b], kv_us.at[p], kv_rcv.at[b], {"ctxo": jnp.minimum(z + 1, nz - 1)})

    def kv_down(p):
        b = 2 * p + m
        return rcopy(kvs.at[b], kvs.at[b], kv_ds.at[p], kv_rcv.at[b], {"ctxo": jnp.maximum(z - 1, 0)})

    def kv_fwd(p):
        b = 2 * p + m
        return rcopy(kvs.at[b], kvs.at[b], kv_fs.at[p], kv_rcv.at[b], sib)

    def kv_wait(b):
        rcopy(kvs.at[b], kvs.at[b], kv_fs.at[0], kv_rcv.at[b], sib).wait_recv()

    kv_fwd(z).start()
    @pl.when(z < nz - 1)
    def _():
        kv_up(z).start()

    if EXTRA:
        @pl.when(z > 0)
        def _():
            kv_down(z).start()

    between = both(z > 0, z < nz - 1)

    def relay(r):
        lo, hi = z - r, z + r

        @pl.when(both(between, lo >= 0))
        def _():
            p = jnp.maximum(lo, 0)
            kv_wait(2 * p + m)
            kv_up(p).start()
            kv_fwd(p).start()

        if EXTRA:
            @pl.when(both(between, hi < nz))
            def _():
                p = jnp.minimum(hi, nz - 1)
                kv_wait(2 * p + m)
                kv_down(p).start()

                if GIVE2:
                    @pl.when(both(z == 1, r == 1))
                    def _():
                        kv_fwd(p).start()

    def give_all(j):
        for r in (0, 1):
            q_give(j, r).start()

    def give_all_d(j):
        for r in (0, 1):
            d_give(j, r).start()

    def prep_kv(b):
        kT[b] = kvs[b, 0].T
        vT[b] = kvs[b, 1].T

    prep_kv(c)
    q_loc[0].wait()

    def prep_q(h):
        @pl.when(h < heads)
        def _():
            q_swap(jnp.minimum(h, heads - 1)).wait_recv()

            @pl.when(h + 2 < n_own)
            def _():
                q_swap(jnp.minimum(h + 2, heads - 1)).start()

            @pl.when(h + 2 == n_own)
            def _():
                loop(n_own, lambda k: d_swap(k).start())

        if EXTRA:
            @pl.when(h >= heads)
            def _():
                for r in (0, 1):
                    q_give(jnp.maximum(h - heads, 0), r).wait_recv()

        qT[h] = qs[h].T

    def tri():
        r = lax.broadcasted_iota(jnp.int32, (tile, tile), 0)
        s = lax.broadcasted_iota(jnp.int32, (tile, tile), 1)
        return s >= r

    def span(t, kind):
        if kind == DIAG:
            return (t + 1) * tile
        return half if kind == SIB and (t + 1) * tile <= half else chip_len

    def cols(t):
        return slice(t * tile, (t + 1) * tile)

    def masked(s, t, kind, fill):
        nk = span(t, kind)
        if kind == DIAG:
            low = jnp.where(tri(), s[nk - tile:], fill)
            return jnp.concatenate([s[:nk - tile], low], axis=0) if nk > tile else low
        if kind == SIB:
            row = lax.broadcasted_iota(jnp.int32, (1, tile), 1) + t * tile
            seen = m * half + jnp.where(row >= half, half, 0)
            return jnp.where(lax.broadcasted_iota(jnp.int32, s.shape, 0) < seen, s, fill)
        return s

    def put_scores(t, kind, s):
        s = masked(s, t, kind, -jnp.inf)
        sb[:span(t, kind), cols(t)] = s
        mbr[:, cols(t)] = jnp.max(s, axis=0, keepdims=True)

    def scores(b, h, t, kind):
        return dot(kvs[b, 0, :span(t, kind), :], qT[h, :, cols(t)])

    def start_scores(b, h, kind):
        for t in range(n_tiles):
            put_scores(t, kind, scores(b, h, t, kind))

    def fwd_step(b, h, kind, bn, hn, kind_n):
        for t in range(n_tiles):
            sl = cols(t)
            nk = span(t, kind)
            top = mbr[:, sl]
            if kind != DIAG:
                old = mr[h, :, sl]
                top = jnp.maximum(old, top)
                fade = jnp.exp2((old - top) * c2)
            s = sb[:nk, sl]
            sn = scores(bn, hn, t, kind_n)
            p = jnp.exp2((s - top) * c2)
            tot = jnp.sum(p, axis=0, keepdims=True)
            o = dot(vT[b, :, :nk], p.astype(BF))
            put_scores(t, kind_n, sn)
            if kind == DIAG:
                lr[h, :, sl] = tot
                oT[h, :, sl] = o
            else:
                lr[h, :, sl] = lr[h, :, sl] * fade + tot
                oT[h, :, sl] = oT[h, :, sl] * fade + o
            mr[h, :, sl] = top

    def fwd_part(part):
        own = part == 0
        zq = jnp.where(own, z, zs)
        h0 = jnp.where(own, 0, heads)
        nh = jnp.where(own, n_own, take)
        cb = 2 * zq + m
        sbk = 2 * zq + 1 - m

        def fwd_block(i):
            b = 2 * (zq - 1 - i // 2) + jnp.where(lax.rem(i, 2) == 0, m, 1 - m)
            return jnp.where(i >= 2 * zq, cb, b)

        def arrive(i):
            b = fwd_block(i)
            p = zq - 1 - i // 2

            @pl.when(both(i < 2 * zq, either(own, p > z)))
            def _():
                column = lax.rem(i, 2) == 0

                @pl.when(jnp.logical_not(both(between, column)))
                def _():
                    kv_wait(b)

                @pl.when(both(jnp.logical_not(between), column))
                def _():
                    kv_fwd(jnp.maximum(p, 0)).start()

                prep_kv(b)

        def plane(n):
            h = h0 + n

            @pl.when(n + 1 < nh)
            def _():
                prep_q(h + 1)

            @pl.when(both(own, n == RELAY1))
            def _():
                relay(1)

            if EXTRA:
                @pl.when(both(own, n == RELAY1))
                def _():
                    loop(give, give_all)

                @pl.when(both(own, n == n_own - 1))
                def _():
                    loop(give, give_all_d)

            fwd_step(cb, h, DIAG, sbk, h, SIB)
            fwd_step(sbk, h, SIB, cb, h0 + jnp.minimum(n + 1, nh - 1), DIAG)

        def full(n):
            i = n // nh
            k = n - i * nh
            last = k == nh - 1

            @pl.when(both(own, n == RELAY2))
            def _():
                relay(2)

            @pl.when(last)
            def _():
                arrive(i + 1)

            fwd_step(fwd_block(i), h0 + k, FULL, fwd_block(jnp.where(last, i + 1, i)), h0 + jnp.where(last, 0, k + 1), FULL)

        @pl.when(nh > 0)
        def _():
            @pl.when(jnp.logical_not(own))
            def _():
                @pl.when(jnp.logical_not(between))
                def _():
                    kv_wait(cb)
                    kv_fwd(zq).start()

                prep_kv(cb)

            prep_q(h0)
            start_scores(cb, h0, DIAG)
            kv_wait(sbk)
            prep_kv(sbk)
            loop(nh, plane)

            @pl.when(zq > 0)
            def _():
                arrive(0)
                start_scores(fwd_block(0), h0, FULL)
                loop(2 * zq * nh, full)

    loop(2 if EXTRA else 1, fwd_part)

    q_loc[1].wait()

    def slot(n):
        return jnp.where(n < n_own, n, n - n_own + heads)

    def fwd_end(n):
        h = slot(n)

        @pl.when(h < heads)
        def _():
            d_swap(jnp.minimum(h, heads - 1)).wait_recv()

        if EXTRA:
            @pl.when(h >= heads)
            def _():
                for r in (0, 1):
                    d_give(jnp.maximum(h - heads, 0), r).wait_recv()

        d = dos[h].T
        doT[h] = d
        l = lr[h]
        o = oT[h] / l
        mr[h] = mr[h] * c2 + jnp.log2(l)
        dr[h] = jnp.sum(o * d.astype(F32), axis=0, keepdims=True)
        os[h] = o.T.astype(BF)
        dqT[h] = jnp.zeros_like(o)

    loop(n_own + take, fwd_end)

    def res_copies(src, dst, loc, snd, rcv, h):
        return (pltpu.make_async_copy(src.at[h, my_rows], dst.at[y, h], loc.at[h]),
                rcopy(src.at[h, peer_rows], dst.at[y, h], snd.at[h], rcv.at[h], peer))

    def o_copies(h):
        return res_copies(os, o_out, o_loc, o_snd, o_rcv, h)

    def dq_copies(h):
        return res_copies(dqs, dq_out, dq_loc, dq_snd, dq_rcv, h)

    def back(src, dst, snd, rcv, j, r, n):
        return rcopy(src.at[heads + j, rows[r]], dst.at[y, heads - n + j], snd.at[j, r], rcv.at[j, r], mates[r])

    def start_both(pair):
        for cp in pair:
            cp.start()

    loop(n_own, lambda h: start_both(o_copies(h)))
    loop(take, lambda j: start_both(back(os, o_out, ho_snd, ho_rcv, j, r, take) for r in (0, 1)))

    def bwd_step(b, h, kind):
        for t in range(n_tiles):
            sl = cols(t)
            nk = span(t, kind)
            s = dot(kvs[b, 0, :nk, :], qT[h, :, sl])
            dp = dot(kvs[b, 1, :nk, :], doT[h, :, sl])
            p = masked(jnp.exp2(s * c2 - mr[h, :, sl]), t, kind, 0.0)
            ds = (p * (dp - dr[h, :, sl])).astype(BF)
            dkv[b, 1, :nk, :] += dot(p.astype(BF), dos[h, sl, :])
            dkv[b, 0, :nk, :] += dot(ds, qs[h, sl, :])
            dqT[h, :, sl] += dot(kT[b, :, :nk], ds)

    def y_send(p):
        return rcopy(dkv.at[2 * p + 1 - m], ybuf.at[p], y_snd.at[p], y_rcv.at[p], sib)

    def y_add(p):
        rcopy(dkv.at[0], ybuf.at[p], y_snd.at[p], y_rcv.at[p], sib).wait_recv()
        dkv[2 * p + m] = dkv[2 * p + m] + ybuf[p]

    def z_send(p):
        return rcopy(dkv.at[2 * p + m], zbuf.at[z], z_snd.at[p], z_rcv.at[z], {"ctxo": p})

    def c_send(p):
        return rcopy(dkv.at[2 * p + m], cbuf.at[p], z_snd.at[p], c_rcv.at[p], {"ctxo": 2})

    def leave(p):
        @pl.when(both(z == 3, p < 2))
        def _():
            c_send(jnp.minimum(p, 1)).start()

        @pl.when(either(both(z == 3, p == 2), z < 2))
        def _():
            z_send(p).start()

    def chain(p):
        rcopy(dkv.at[0], cbuf.at[p], z_snd.at[p], c_rcv.at[p], {"ctxo": 2}).wait_recv()
        dkv[2 * p + m] = dkv[2 * p + m] + cbuf[p]
        z_send(p).start()

    def finish_dq(h):
        dqs[h] = (dqT[h] * scale).T.astype(BF)

    n_planes = jnp.where(helps, zs, z)

    def bwd_full(i):
        k = i // 2
        p = jnp.where(helps, n_planes - 1 - k, k)
        first = lax.rem(i, 2) == 0
        b = 2 * p + jnp.where(first, 1 - m, m)
        na = jnp.where(p < z, n_own, 0)
        nb = take

        def one(n):
            bwd_step(b, jnp.where(n < na, n, n - na + heads), FULL)

        loop(na + nb, one)

        @pl.when(both(first, p != z))
        def _():
            y_send(p).start()

        if EXTRA:
            @pl.when(both(helps, i == 0))
            def _():
                y_add(zs)
                leave(zs)

        @pl.when(both(jnp.logical_not(first), p != z))
        def _():
            y_add(p)
            leave(p)

        @pl.when(both(z == 2, i == 2))
        def _():
            chain(0)

    def bwd_part(part):
        own = part == 1
        zq = jnp.where(own, z, zs)
        h0 = jnp.where(own, 0, heads)

        def plane(n):
            h = h0 + n
            bwd_step(2 * zq + 1 - m, h, SIB)
            bwd_step(2 * zq + m, h, DIAG)

            @pl.when(own)
            def _():
                finish_dq(h)

                @pl.when(h > 0)
                def _():
                    start_both(dq_copies(jnp.clip(h - 1, 0, heads - 1)))

                @pl.when(both(z == 2, h == 1))
                def _():
                    chain(1)

        loop(jnp.where(own, n_own, take), plane)

        @pl.when(either(own, helps))
        def _():
            y_send(zq).start()

        @pl.when(jnp.logical_not(own))
        def _():
            loop(2 * n_planes, bwd_full)

            def taken_dq(j):
                finish_dq(heads + j)

            loop(take, taken_dq)
            loop(take, lambda j: start_both(back(dqs, dq_out, hg_snd, hg_rcv, j, r, take) for r in (0, 1)))

    loop(2, bwd_part)
    start_both(dq_copies(n_own - 1))

    def z_comes(t):
        if t == 3:
            return z == 2
        if t == 2:
            return z < 2
        if t == 1:
            return either(z == 0, z == 2) if GIVE2 else z == 0
        return z > 0 if GIVE3 else z < 0

    for t in range(nz):
        @pl.when(z_comes(t))
        def _():
            rcopy(dkv.at[0], zbuf.at[t], z_snd.at[0], z_rcv.at[t], {"ctxo": t}).wait_recv()
            dkv[c] = dkv[c] + zbuf[t]

    y_add(z)
    gs[0] = (dkv[c, 0] * scale).astype(BF)
    gs[1] = dkv[c, 1].astype(BF)
    outs = (dk_out, dv_out)
    g_copies = []
    for i in (0, 1):
        g_copies.append((pltpu.make_async_copy(gs.at[i, my_rows], outs[i].at[y], g_loc.at[i]),
                         rcopy(gs.at[i, peer_rows], outs[i].at[y], g_snd.at[i], g_rcv.at[i], peer)))
        start_both(g_copies[-1])

    for i in (0, 1):
        kv_swap(i)[0].wait_send()

    def own_sent(h):
        q_swap(h).wait_send()
        d_swap(h).wait_send()
        for a, b in (o_copies(h), dq_copies(h)):
            a.wait()
            b.wait()

    loop(n_own, own_sent)

    def given(j):
        for r in (0, 1):
            q_give(j, r).wait_send()
            d_give(j, r).wait_send()
            for dst, snd, rcv in ((o_out, ho_snd, ho_rcv), (dq_out, hg_snd, hg_rcv)):
                rcopy(os.at[0, my_rows], dst.at[batch[r], heads - give + j], snd.at[j, r], rcv.at[j, r], mates[r]).wait_recv()

    def taken(j):
        for r in (0, 1):
            back(os, o_out, ho_snd, ho_rcv, j, r, take).wait_send()
            back(dqs, dq_out, hg_snd, hg_rcv, j, r, take).wait_send()

    if EXTRA:
        loop(give, given)
        loop(take, taken)

    @pl.when(z < nz - 1)
    def _():
        loop(z + 1, lambda p: kv_up(p).wait_send())

    if EXTRA:
        @pl.when(z > 0)
        def _():
            loop(nz - z, lambda k: kv_down(z + k).wait_send())

    def planes_sent(p):
        kv_fwd(p).wait_send()
        y_send(p).wait_send()

        @pl.when(p != z)
        def _():
            z_send(p).wait_send()

    loop(jnp.where(helps, zs, z) + 1, planes_sent)
    for a, b in g_copies:
        a.wait()
        b.wait()


def solution(mesh):
    nz = mesh.shape["ctxo"]
    spec = P("data", ("ctxo", "ctx"), None, None)

    def local(q, k, v, do):
        rows, half, heads, dim = q.shape
        n = 2 * half
        nb = 2 * nz
        nh = heads + EXTRA
        ex = max(EXTRA, 1)
        q, do = jnp.swapaxes(q, 1, 2), jnp.swapaxes(do, 1, 2)
        k, v = k[:, :, 0], v[:, :, 0]
        hbm = pl.BlockSpec(memory_space=pl.ANY)
        S = jax.ShapeDtypeStruct
        V = pltpu.VMEM

        def dma(*shape):
            return pltpu.SemaphoreType.DMA(shape)

        o, dq, dk, dv = pl.pallas_call(
            functools.partial(kernel, heads),
            out_shape=[S(q.shape, BF), S(q.shape, BF), S(k.shape, BF), S(k.shape, BF)],
            in_specs=[hbm] * 4,
            out_specs=[hbm] * 4,
            scratch_shapes=[
                V((nh, n, dim), BF), V((nh, n, dim), BF), V((nh, dim, n), BF), V((nh, dim, n), BF),
                V((nb, 2, n, dim), BF), V((nb, dim, n), BF), V((nb, dim, n), BF),
                V((nh, dim, n), F32), V((nh, dim, n), F32),
                V((nh, 1, n), F32), V((nh, 1, n), F32), V((nh, 1, n), F32),
                V((n, n), F32), V((1, n), F32),
                V((nb, 2, n, dim), F32), V((nz, 2, n, dim), F32), V((nz, 2, n, dim), F32), V((2, 2, n, dim), F32),
                V((nh, n, dim), BF), V((nh, n, dim), BF), V((2, n, dim), BF),
                dma(2), dma(2), dma(2), dma(2), dma(heads), dma(heads), dma(heads), dma(heads),
                dma(ex, 2), dma(ex, 2), dma(ex, 2), dma(ex, 2),
                dma(nz), dma(nz), dma(nz), dma(nb), dma(nz), dma(nz), dma(nz), dma(nz), dma(2),
                dma(heads), dma(heads), dma(heads), dma(heads), dma(heads), dma(heads),
                dma(ex, 2), dma(ex, 2), dma(ex, 2), dma(ex, 2), dma(2), dma(2), dma(2),
            ],
            compiler_params=pltpu.CompilerParams(collective_id=0, has_side_effects=True, vmem_limit_bytes=62 * 1024 * 1024),
            name="attn",
        )(q, do, k, v)
        return jnp.swapaxes(o, 1, 2), jnp.swapaxes(dq, 1, 2), dk[:, :, None], dv[:, :, None]

    return jax.shard_map(local, mesh=mesh, in_specs=(spec,) * 4, out_specs=(spec,) * 4, check_vma=False)
```

```python
import functools
import math

import jax
import jax.numpy as jnp
from jax import lax
from jax.experimental import pallas as pl
from jax.experimental.pallas import tpu as pltpu
from jax.sharding import PartitionSpec as P

MESH = pl.DeviceIdType.MESH
BF = jnp.bfloat16
F32 = jnp.float32
DIAG, SIB, FULL = 0, 1, 2
EXTRA = 2
RELAY1, RELAY2 = 3, 4


def dot(a, b):
    return jnp.dot(a, b, preferred_element_type=F32)


def either(*conds):
    return functools.reduce(jnp.logical_or, conds)


def both(*conds):
    return functools.reduce(jnp.logical_and, conds)


def loop(n, body):
    def step(i, carry):
        body(i)
        return carry

    lax.fori_loop(0, n, step, 0)


def kernel(heads, q_in, do_in, k_in, v_in, o_out, dq_out, dk_out, dv_out,
           qs, dos, qT, doT, kvs, kT, vT, oT, dqT, mr, lr, dr, sb, mbr, dkv, ybuf, zbuf, cbuf, os, dqs, gs,
           kv_loc, kv_snd, kv_xrc, qd_loc, q_snd, q_rcv, d_snd, d_rcv, hq_snd, hq_rcv, hd_snd, hd_rcv,
           kv_us, kv_ds, kv_fs, kv_rcv, y_snd, y_rcv, z_snd, z_rcv, c_rcv,
           o_loc, o_snd, o_rcv, dq_loc, dq_snd, dq_rcv, ho_snd, ho_rcv, hg_snd, hg_rcv, g_loc, g_snd, g_rcv):
    _, chip_len, dim = qs.shape
    nz = 4
    half = chip_len // 2
    tile = min(256, chip_len)
    n_tiles = chip_len // tile
    scale = 1.0 / math.sqrt(dim)
    c2 = scale * math.log2(math.e)

    z = lax.axis_index("ctxo")
    x = lax.axis_index("ctx")
    m = lax.rem(x, 2)
    y = x // 2
    zs = lax.rem(z + 2, nz)
    give = jnp.where(z == 3, EXTRA, 0)
    take = jnp.where(z == 1, EXTRA, 0)
    n_own = heads - give
    helps = take > 0
    c = 2 * z + m
    peer = {"ctx": 2 * (1 - y) + m}
    sib = {"ctx": 2 * y + 1 - m}
    mates = ({"ctxo": zs}, {"ctxo": zs, "ctx": 2 * (1 - y) + m})
    my_rows = pl.ds(pl.multiple_of(y * half, half), half)
    peer_rows = pl.ds(pl.multiple_of((1 - y) * half, half), half)
    batch = (y, 1 - y)
    rows = (my_rows, peer_rows)

    def rcopy(src, dst, ss, rs, dev):
        return pltpu.make_async_remote_copy(src_ref=src, dst_ref=dst, send_sem=ss, recv_sem=rs, device_id=dev, device_id_type=MESH)

    bar = pltpu.get_barrier_semaphore()
    for dev in (peer, sib, mates[1]) + tuple({"ctxo": lax.rem(z + d, nz)} for d in range(1, nz)):
        pl.semaphore_signal(bar, inc=1, device_id=dev, device_id_type=MESH)
    pl.semaphore_wait(bar, nz + 2)

    def kv_swap(i):
        src = (k_in, v_in)[i]
        return (rcopy(src.at[1 - y], kvs.at[c, i, my_rows], kv_snd.at[i], kv_xrc.at[i], peer),
                pltpu.make_async_copy(src.at[y], kvs.at[c, i, my_rows], kv_loc.at[i]))

    def q_swap(h):
        return rcopy(q_in.at[1 - y, h], qs.at[h, my_rows], q_snd.at[h], q_rcv.at[h], peer)

    def d_swap(h):
        return rcopy(do_in.at[1 - y, h], dos.at[h, my_rows], d_snd.at[h], d_rcv.at[h], peer)

    def q_give(j, r):
        return rcopy(q_in.at[batch[r], jnp.minimum(heads - give + j, heads - 1)], qs.at[heads + j, my_rows], hq_snd.at[j, r], hq_rcv.at[j, r], mates[r])

    def d_give(j, r):
        return rcopy(do_in.at[batch[r], jnp.minimum(heads - give + j, heads - 1)], dos.at[heads + j, my_rows], hd_snd.at[j, r], hd_rcv.at[j, r], mates[r])

    for i in (0, 1):
        for cp in kv_swap(i):
            cp.start()
    q_loc = (pltpu.make_async_copy(q_in.at[y], qs.at[:heads, my_rows], qd_loc.at[0]),
             pltpu.make_async_copy(do_in.at[y], dos.at[:heads, my_rows], qd_loc.at[1]))
    for cp in q_loc:
        cp.start()
    dkv[...] = jnp.zeros_like(dkv)
    for i in (0, 1):
        swap, local = kv_swap(i)
        local.wait()
        swap.wait_recv()
    for h in (0, 1):
        q_swap(h).start()

    def kv_up(p):
        b = 2 * p + m
        return rcopy(kvs.at[b], kvs.at[b], kv_us.at[p], kv_rcv.at[b], {"ctxo": jnp.minimum(z + 1, nz - 1)})

    def kv_down(p):
        b = 2 * p + m
        return rcopy(kvs.at[b], kvs.at[b], kv_ds.at[p], kv_rcv.at[b], {"ctxo": jnp.maximum(z - 1, 0)})

    def kv_fwd(p):
        b = 2 * p + m
        return rcopy(kvs.at[b], kvs.at[b], kv_fs.at[p], kv_rcv.at[b], sib)

    def kv_wait(b):
        rcopy(kvs.at[b], kvs.at[b], kv_fs.at[0], kv_rcv.at[b], sib).wait_recv()

    kv_fwd(z).start()
    @pl.when(z < nz - 1)
    def _():
        kv_up(z).start()

    if EXTRA:
        @pl.when(z >= 2)
        def _():
            kv_down(z).start()

    between = both(z > 0, z < nz - 1)

    def relay(r):
        lo, hi = z - r, z + r

        @pl.when(both(between, lo >= 0))
        def _():
            p = jnp.maximum(lo, 0)
            kv_wait(2 * p + m)
            kv_up(p).start()
            kv_fwd(p).start()

        if EXTRA:
            @pl.when(both(z == 2, hi < nz))
            def _():
                p = jnp.minimum(hi, nz - 1)
                kv_wait(2 * p + m)
                kv_down(p).start()

    def give_all(j):
        for r in (0, 1):
            q_give(j, r).start()

    def give_all_d(j):
        for r in (0, 1):
            d_give(j, r).start()

    def prep_kv(b):
        kT[b] = kvs[b, 0].T
        vT[b] = kvs[b, 1].T

    prep_kv(c)
    q_loc[0].wait()

    def prep_q(h):
        @pl.when(h < heads)
        def _():
            q_swap(jnp.minimum(h, heads - 1)).wait_recv()

            @pl.when(h + 2 < n_own)
            def _():
                q_swap(jnp.minimum(h + 2, heads - 1)).start()

            @pl.when(h + 2 == n_own)
            def _():
                loop(n_own, lambda k: d_swap(k).start())

        if EXTRA:
            @pl.when(h >= heads)
            def _():
                for r in (0, 1):
                    q_give(jnp.maximum(h - heads, 0), r).wait_recv()

        qT[h] = qs[h].T

    def tri():
        r = lax.broadcasted_iota(jnp.int32, (tile, tile), 0)
        s = lax.broadcasted_iota(jnp.int32, (tile, tile), 1)
        return s >= r

    def span(t, kind):
        if kind == DIAG:
            return (t + 1) * tile
        return half if kind == SIB and (t + 1) * tile <= half else chip_len

    def cols(t):
        return slice(t * tile, (t + 1) * tile)

    def masked(s, t, kind, fill):
        nk = span(t, kind)
        if kind == DIAG:
            low = jnp.where(tri(), s[nk - tile:], fill)
            return jnp.concatenate([s[:nk - tile], low], axis=0) if nk > tile else low
        if kind == SIB:
            row = lax.broadcasted_iota(jnp.int32, (1, tile), 1) + t * tile
            seen = m * half + jnp.where(row >= half, half, 0)
            return jnp.where(lax.broadcasted_iota(jnp.int32, s.shape, 0) < seen, s, fill)
        return s

    def put_scores(t, kind, s):
        s = masked(s, t, kind, -jnp.inf)
        sb[:span(t, kind), cols(t)] = s
        mbr[:, cols(t)] = jnp.max(s, axis=0, keepdims=True)

    def scores(b, h, t, kind):
        return dot(kvs[b, 0, :span(t, kind), :], qT[h, :, cols(t)])

    def start_scores(b, h, kind):
        for t in range(n_tiles):
            put_scores(t, kind, scores(b, h, t, kind))

    def fwd_step(b, h, kind, bn, hn, kind_n):
        for t in range(n_tiles):
            sl = cols(t)
            nk = span(t, kind)
            top = mbr[:, sl]
            if kind != DIAG:
                old = mr[h, :, sl]
                top = jnp.maximum(old, top)
                fade = jnp.exp2((old - top) * c2)
            s = sb[:nk, sl]
            sn = scores(bn, hn, t, kind_n)
            p = jnp.exp2((s - top) * c2)
            tot = jnp.sum(p, axis=0, keepdims=True)
            o = dot(vT[b, :, :nk], p.astype(BF))
            put_scores(t, kind_n, sn)
            if kind == DIAG:
                lr[h, :, sl] = tot
                oT[h, :, sl] = o
            else:
                lr[h, :, sl] = lr[h, :, sl] * fade + tot
                oT[h, :, sl] = oT[h, :, sl] * fade + o
            mr[h, :, sl] = top

    def fwd_part(part):
        own = part == 0
        zq = jnp.where(own, z, zs)
        h0 = jnp.where(own, 0, heads)
        nh = jnp.where(own, n_own, take)
        cb = 2 * zq + m
        sbk = 2 * zq + 1 - m

        def fwd_block(i):
            b = 2 * (zq - 1 - i // 2) + jnp.where(lax.rem(i, 2) == 0, m, 1 - m)
            return jnp.where(i >= 2 * zq, cb, b)

        def arrive(i):
            b = fwd_block(i)
            p = zq - 1 - i // 2

            @pl.when(both(i < 2 * zq, either(own, p > z)))
            def _():
                column = lax.rem(i, 2) == 0
                relayed = both(between, column, p < z)

                @pl.when(jnp.logical_not(relayed))
                def _():
                    kv_wait(b)

                @pl.when(both(jnp.logical_not(relayed), column))
                def _():
                    kv_fwd(jnp.maximum(p, 0)).start()

                prep_kv(b)

        def plane(n):
            h = h0 + n

            @pl.when(n + 1 < nh)
            def _():
                prep_q(h + 1)

            @pl.when(both(own, n == RELAY1))
            def _():
                relay(1)

            if EXTRA:
                @pl.when(both(own, n == RELAY1))
                def _():
                    loop(give, give_all)

                @pl.when(both(own, n == n_own - 1))
                def _():
                    loop(give, give_all_d)

            fwd_step(cb, h, DIAG, sbk, h, SIB)
            fwd_step(sbk, h, SIB, cb, h0 + jnp.minimum(n + 1, nh - 1), DIAG)

        def full(n):
            i = n // nh
            k = n - i * nh
            last = k == nh - 1

            @pl.when(both(own, n == RELAY2))
            def _():
                relay(2)

            @pl.when(last)
            def _():
                arrive(i + 1)

            fwd_step(fwd_block(i), h0 + k, FULL, fwd_block(jnp.where(last, i + 1, i)), h0 + jnp.where(last, 0, k + 1), FULL)

        @pl.when(nh > 0)
        def _():
            @pl.when(jnp.logical_not(own))
            def _():
                kv_wait(cb)
                kv_fwd(zq).start()
                prep_kv(cb)

            prep_q(h0)
            start_scores(cb, h0, DIAG)
            kv_wait(sbk)
            prep_kv(sbk)
            loop(nh, plane)

            @pl.when(zq > 0)
            def _():
                arrive(0)
                start_scores(fwd_block(0), h0, FULL)
                loop(2 * zq * nh, full)

    loop(2 if EXTRA else 1, fwd_part)

    q_loc[1].wait()

    def slot(n):
        return jnp.where(n < n_own, n, n - n_own + heads)

    def fwd_end(n):
        h = slot(n)

        @pl.when(h < heads)
        def _():
            d_swap(jnp.minimum(h, heads - 1)).wait_recv()

        if EXTRA:
            @pl.when(h >= heads)
            def _():
                for r in (0, 1):
                    d_give(jnp.maximum(h - heads, 0), r).wait_recv()

        d = dos[h].T
        doT[h] = d
        l = lr[h]
        o = oT[h] / l
        mr[h] = mr[h] * c2 + jnp.log2(l)
        dr[h] = jnp.sum(o * d.astype(F32), axis=0, keepdims=True)
        os[h] = o.T.astype(BF)
        dqT[h] = jnp.zeros_like(o)

    loop(n_own + take, fwd_end)

    def res_copies(src, dst, loc, snd, rcv, h):
        return (pltpu.make_async_copy(src.at[h, my_rows], dst.at[y, h], loc.at[h]),
                rcopy(src.at[h, peer_rows], dst.at[y, h], snd.at[h], rcv.at[h], peer))

    def o_copies(h):
        return res_copies(os, o_out, o_loc, o_snd, o_rcv, h)

    def dq_copies(h):
        return res_copies(dqs, dq_out, dq_loc, dq_snd, dq_rcv, h)

    def back(src, dst, snd, rcv, j, r, n):
        return rcopy(src.at[heads + j, rows[r]], dst.at[y, heads - n + j], snd.at[j, r], rcv.at[j, r], mates[r])

    def start_both(pair):
        for cp in pair:
            cp.start()

    loop(n_own, lambda h: start_both(o_copies(h)))
    loop(take, lambda j: start_both(back(os, o_out, ho_snd, ho_rcv, j, r, take) for r in (0, 1)))

    def bwd_step(b, h, kind):
        for t in range(n_tiles):
            sl = cols(t)
            nk = span(t, kind)
            s = dot(kvs[b, 0, :nk, :], qT[h, :, sl])
            dp = dot(kvs[b, 1, :nk, :], doT[h, :, sl])
            p = masked(jnp.exp2(s * c2 - mr[h, :, sl]), t, kind, 0.0)
            ds = (p * (dp - dr[h, :, sl])).astype(BF)
            dkv[b, 1, :nk, :] += dot(p.astype(BF), dos[h, sl, :])
            dkv[b, 0, :nk, :] += dot(ds, qs[h, sl, :])
            dqT[h, :, sl] += dot(kT[b, :, :nk], ds)

    def y_send(p):
        return rcopy(dkv.at[2 * p + 1 - m], ybuf.at[p], y_snd.at[p], y_rcv.at[p], sib)

    def y_add(p):
        rcopy(dkv.at[0], ybuf.at[p], y_snd.at[p], y_rcv.at[p], sib).wait_recv()
        dkv[2 * p + m] = dkv[2 * p + m] + ybuf[p]

    def z_send(p):
        return rcopy(dkv.at[2 * p + m], zbuf.at[z], z_snd.at[p], z_rcv.at[z], {"ctxo": p})

    def c_send(p):
        return rcopy(dkv.at[2 * p + m], cbuf.at[p], z_snd.at[p], c_rcv.at[p], {"ctxo": 2})

    def leave(p):
        @pl.when(both(z == 3, p < 2))
        def _():
            c_send(jnp.minimum(p, 1)).start()

        @pl.when(either(both(z == 3, p == 2), z < 2))
        def _():
            z_send(p).start()

    def chain(p):
        rcopy(dkv.at[0], cbuf.at[p], z_snd.at[p], c_rcv.at[p], {"ctxo": 2}).wait_recv()
        dkv[2 * p + m] = dkv[2 * p + m] + cbuf[p]
        z_send(p).start()

    def finish_dq(h):
        dqs[h] = (dqT[h] * scale).T.astype(BF)

    n_planes = jnp.where(helps, zs, z)

    def bwd_full(i):
        k = i // 2
        p = jnp.where(helps, n_planes - 1 - k, k)
        first = lax.rem(i, 2) == 0
        b = 2 * p + jnp.where(first, 1 - m, m)
        na = jnp.where(p < z, n_own, 0)
        nb = take

        def one(n):
            bwd_step(b, jnp.where(n < na, n, n - na + heads), FULL)

        loop(na + nb, one)

        @pl.when(both(first, p != z))
        def _():
            y_send(p).start()

        if EXTRA:
            @pl.when(both(helps, i == 0))
            def _():
                y_add(zs)
                leave(zs)

        @pl.when(both(jnp.logical_not(first), p != z))
        def _():
            y_add(p)
            leave(p)

        @pl.when(both(z == 2, i == 2))
        def _():
            chain(0)

    def bwd_part(part):
        own = part == 1
        zq = jnp.where(own, z, zs)
        h0 = jnp.where(own, 0, heads)

        def plane(n):
            h = h0 + n
            bwd_step(2 * zq + 1 - m, h, SIB)
            bwd_step(2 * zq + m, h, DIAG)

            @pl.when(own)
            def _():
                finish_dq(h)

                @pl.when(h > 0)
                def _():
                    start_both(dq_copies(jnp.clip(h - 1, 0, heads - 1)))

                @pl.when(both(z == 2, h == 1))
                def _():
                    chain(1)

        loop(jnp.where(own, n_own, take), plane)

        @pl.when(either(own, helps))
        def _():
            y_send(zq).start()

        @pl.when(jnp.logical_not(own))
        def _():
            loop(2 * n_planes, bwd_full)

            def taken_dq(j):
                finish_dq(heads + j)

            loop(take, taken_dq)
            loop(take, lambda j: start_both(back(dqs, dq_out, hg_snd, hg_rcv, j, r, take) for r in (0, 1)))

    loop(2, bwd_part)
    start_both(dq_copies(n_own - 1))

    def z_comes(t):
        if t == 3:
            return z == 2
        if t == 2:
            return z < 2
        if t == 1:
            return z != 1 if EXTRA else z == 0
        return z < 0

    for t in range(nz):
        @pl.when(z_comes(t))
        def _():
            rcopy(dkv.at[0], zbuf.at[t], z_snd.at[0], z_rcv.at[t], {"ctxo": t}).wait_recv()
            dkv[c] = dkv[c] + zbuf[t]

    y_add(z)
    gs[0] = (dkv[c, 0] * scale).astype(BF)
    gs[1] = dkv[c, 1].astype(BF)
    outs = (dk_out, dv_out)
    g_copies = []
    for i in (0, 1):
        g_copies.append((pltpu.make_async_copy(gs.at[i, my_rows], outs[i].at[y], g_loc.at[i]),
                         rcopy(gs.at[i, peer_rows], outs[i].at[y], g_snd.at[i], g_rcv.at[i], peer)))
        start_both(g_copies[-1])

    for i in (0, 1):
        kv_swap(i)[0].wait_send()

    def own_sent(h):
        q_swap(h).wait_send()
        d_swap(h).wait_send()
        for a, b in (o_copies(h), dq_copies(h)):
            a.wait()
            b.wait()

    loop(n_own, own_sent)

    def given(j):
        for r in (0, 1):
            q_give(j, r).wait_send()
            d_give(j, r).wait_send()
            for dst, snd, rcv in ((o_out, ho_snd, ho_rcv), (dq_out, hg_snd, hg_rcv)):
                rcopy(os.at[0, my_rows], dst.at[batch[r], heads - give + j], snd.at[j, r], rcv.at[j, r], mates[r]).wait_recv()

    def taken(j):
        for r in (0, 1):
            back(os, o_out, ho_snd, ho_rcv, j, r, take).wait_send()
            back(dqs, dq_out, hg_snd, hg_rcv, j, r, take).wait_send()

    if EXTRA:
        loop(give, given)
        loop(take, taken)

    @pl.when(z < nz - 1)
    def _():
        loop(z + 1, lambda p: kv_up(p).wait_send())

    if EXTRA:
        @pl.when(z >= 2)
        def _():
            loop(nz - z, lambda k: kv_down(z + k).wait_send())

    def planes_sent(p):
        kv_fwd(p).wait_send()
        y_send(p).wait_send()

        @pl.when(p != z)
        def _():
            z_send(p).wait_send()

    loop(jnp.where(helps, zs, z) + 1, planes_sent)
    for a, b in g_copies:
        a.wait()
        b.wait()


def solution(mesh):
    nz = mesh.shape["ctxo"]
    spec = P("data", ("ctxo", "ctx"), None, None)

    def local(q, k, v, do):
        rows, half, heads, dim = q.shape
        n = 2 * half
        nb = 2 * nz
        nh = heads + EXTRA
        ex = max(EXTRA, 1)
        q, do = jnp.swapaxes(q, 1, 2), jnp.swapaxes(do, 1, 2)
        k, v = k[:, :, 0], v[:, :, 0]
        hbm = pl.BlockSpec(memory_space=pl.ANY)
        S = jax.ShapeDtypeStruct
        V = pltpu.VMEM

        def dma(*shape):
            return pltpu.SemaphoreType.DMA(shape)

        o, dq, dk, dv = pl.pallas_call(
            functools.partial(kernel, heads),
            out_shape=[S(q.shape, BF), S(q.shape, BF), S(k.shape, BF), S(k.shape, BF)],
            in_specs=[hbm] * 4,
            out_specs=[hbm] * 4,
            scratch_shapes=[
                V((nh, n, dim), BF), V((nh, n, dim), BF), V((nh, dim, n), BF), V((nh, dim, n), BF),
                V((nb, 2, n, dim), BF), V((nb, dim, n), BF), V((nb, dim, n), BF),
                V((nh, dim, n), F32), V((nh, dim, n), F32),
                V((nh, 1, n), F32), V((nh, 1, n), F32), V((nh, 1, n), F32),
                V((n, n), F32), V((1, n), F32),
                V((nb, 2, n, dim), F32), V((nz, 2, n, dim), F32), V((nz, 2, n, dim), F32), V((2, 2, n, dim), F32),
                V((nh, n, dim), BF), V((nh, n, dim), BF), V((2, n, dim), BF),
                dma(2), dma(2), dma(2), dma(2), dma(heads), dma(heads), dma(heads), dma(heads),
                dma(ex, 2), dma(ex, 2), dma(ex, 2), dma(ex, 2),
                dma(nz), dma(nz), dma(nz), dma(nb), dma(nz), dma(nz), dma(nz), dma(nz), dma(2),
                dma(heads), dma(heads), dma(heads), dma(heads), dma(heads), dma(heads),
                dma(ex, 2), dma(ex, 2), dma(ex, 2), dma(ex, 2), dma(2), dma(2), dma(2),
            ],
            compiler_params=pltpu.CompilerParams(collective_id=0, has_side_effects=True, vmem_limit_bytes=62 * 1024 * 1024),
            name="attn",
        )(q, do, k, v)
        return jnp.swapaxes(o, 1, 2), jnp.swapaxes(dq, 1, 2), dk[:, :, None], dv[:, :, None]

    return jax.shard_map(local, mesh=mesh, in_specs=(spec,) * 4, out_specs=(spec,) * 4, check_vma=False)
```

```python
import functools
import math

import jax
import jax.numpy as jnp
from jax import lax
from jax.experimental import pallas as pl
from jax.experimental.pallas import tpu as pltpu
from jax.sharding import PartitionSpec as P

MESH = pl.DeviceIdType.MESH
BF = jnp.bfloat16
F32 = jnp.float32
DIAG, SIB, FULL = 0, 1, 2
EXTRA = 1
RELAY1, RELAY2 = 3, 4


def dot(a, b):
    return jnp.dot(a, b, preferred_element_type=F32)


def either(*conds):
    return functools.reduce(jnp.logical_or, conds)


def both(*conds):
    return functools.reduce(jnp.logical_and, conds)


def loop(n, body):
    def step(i, carry):
        body(i)
        return carry

    lax.fori_loop(0, n, step, 0)


def kernel(heads, q_in, do_in, k_in, v_in, o_out, dq_out, dk_out, dv_out,
           qs, dos, qT, doT, kvs, kT, vT, oT, dqT, mr, lr, dr, sb, mbr, dkv, ybuf, zbuf, cbuf, os, dqs, gs,
           kv_loc, kv_snd, kv_xrc, qd_loc, q_snd, q_rcv, d_snd, d_rcv, hq_snd, hq_rcv, hd_snd, hd_rcv,
           kv_us, kv_ds, kv_fs, kv_rcv, y_snd, y_rcv, z_snd, z_rcv, c_rcv,
           o_loc, o_snd, o_rcv, dq_loc, dq_snd, dq_rcv, ho_snd, ho_rcv, hg_snd, hg_rcv, g_loc, g_snd, g_rcv):
    _, chip_len, dim = qs.shape
    nz = 4
    half = chip_len // 2
    tile = min(256, chip_len)
    n_tiles = chip_len // tile
    scale = 1.0 / math.sqrt(dim)
    c2 = scale * math.log2(math.e)

    z = lax.axis_index("ctxo")
    x = lax.axis_index("ctx")
    m = lax.rem(x, 2)
    y = x // 2
    zs = lax.rem(z + 2, nz)
    give = jnp.where(z == 3, EXTRA, 0)
    take = jnp.where(z == 1, EXTRA, 0)
    n_own = heads - give
    helps = take > 0
    c = 2 * z + m
    peer = {"ctx": 2 * (1 - y) + m}
    sib = {"ctx": 2 * y + 1 - m}
    mates = ({"ctxo": zs}, {"ctxo": zs, "ctx": 2 * (1 - y) + m})
    my_rows = pl.ds(pl.multiple_of(y * half, half), half)
    peer_rows = pl.ds(pl.multiple_of((1 - y) * half, half), half)
    batch = (y, 1 - y)
    rows = (my_rows, peer_rows)

    def rcopy(src, dst, ss, rs, dev):
        return pltpu.make_async_remote_copy(src_ref=src, dst_ref=dst, send_sem=ss, recv_sem=rs, device_id=dev, device_id_type=MESH)

    bar = pltpu.get_barrier_semaphore()
    for dev in (peer, sib, mates[1]) + tuple({"ctxo": lax.rem(z + d, nz)} for d in range(1, nz)):
        pl.semaphore_signal(bar, inc=1, device_id=dev, device_id_type=MESH)
    pl.semaphore_wait(bar, nz + 2)

    def kv_swap(i):
        src = (k_in, v_in)[i]
        return (rcopy(src.at[1 - y], kvs.at[c, i, my_rows], kv_snd.at[i], kv_xrc.at[i], peer),
                pltpu.make_async_copy(src.at[y], kvs.at[c, i, my_rows], kv_loc.at[i]))

    def q_swap(h):
        return rcopy(q_in.at[1 - y, h], qs.at[h, my_rows], q_snd.at[h], q_rcv.at[h], peer)

    def d_swap(h):
        return rcopy(do_in.at[1 - y, h], dos.at[h, my_rows], d_snd.at[h], d_rcv.at[h], peer)

    def q_give(j, r):
        return rcopy(q_in.at[batch[r], jnp.minimum(heads - give + j, heads - 1)], qs.at[heads + j, my_rows], hq_snd.at[j, r], hq_rcv.at[j, r], mates[r])

    def d_give(j, r):
        return rcopy(do_in.at[batch[r], jnp.minimum(heads - give + j, heads - 1)], dos.at[heads + j, my_rows], hd_snd.at[j, r], hd_rcv.at[j, r], mates[r])

    for i in (0, 1):
        for cp in kv_swap(i):
            cp.start()
    q_loc = (pltpu.make_async_copy(q_in.at[y], qs.at[:heads, my_rows], qd_loc.at[0]),
             pltpu.make_async_copy(do_in.at[y], dos.at[:heads, my_rows], qd_loc.at[1]))
    for cp in q_loc:
        cp.start()
    dkv[...] = jnp.zeros_like(dkv)
    for i in (0, 1):
        swap, local = kv_swap(i)
        local.wait()
        swap.wait_recv()
    for h in (0, 1):
        q_swap(h).start()

    def kv_up(p):
        b = 2 * p + m
        return rcopy(kvs.at[b], kvs.at[b], kv_us.at[p], kv_rcv.at[b], {"ctxo": jnp.minimum(z + 1, nz - 1)})

    def kv_down(p):
        b = 2 * p + m
        return rcopy(kvs.at[b], kvs.at[b], kv_ds.at[p], kv_rcv.at[b], {"ctxo": jnp.maximum(z - 1, 0)})

    def kv_fwd(p):
        b = 2 * p + m
        return rcopy(kvs.at[b], kvs.at[b], kv_fs.at[p], kv_rcv.at[b], sib)

    def kv_wait(b):
        rcopy(kvs.at[b], kvs.at[b], kv_fs.at[0], kv_rcv.at[b], sib).wait_recv()

    kv_fwd(z).start()
    @pl.when(z < nz - 1)
    def _():
        kv_up(z).start()

    if EXTRA:
        @pl.when(z >= 2)
        def _():
            kv_down(z).start()

    between = both(z > 0, z < nz - 1)

    def relay(r):
        lo, hi = z - r, z + r

        @pl.when(both(between, lo >= 0))
        def _():
            p = jnp.maximum(lo, 0)
            kv_wait(2 * p + m)
            kv_up(p).start()
            kv_fwd(p).start()

        if EXTRA:
            @pl.when(both(z == 2, hi < nz))
            def _():
                p = jnp.minimum(hi, nz - 1)
                kv_wait(2 * p + m)
                kv_down(p).start()

    def give_all(j):
        for r in (0, 1):
            q_give(j, r).start()

    def give_all_d(j):
        for r in (0, 1):
            d_give(j, r).start()

    def prep_kv(b):
        kT[b] = kvs[b, 0].T
        vT[b] = kvs[b, 1].T

    prep_kv(c)
    q_loc[0].wait()

    def prep_q(h):
        @pl.when(h < heads)
        def _():
            q_swap(jnp.minimum(h, heads - 1)).wait_recv()

            @pl.when(h + 2 < n_own)
            def _():
                q_swap(jnp.minimum(h + 2, heads - 1)).start()

            @pl.when(h + 2 == n_own)
            def _():
                loop(n_own, lambda k: d_swap(k).start())

        if EXTRA:
            @pl.when(h >= heads)
            def _():
                for r in (0, 1):
                    q_give(jnp.maximum(h - heads, 0), r).wait_recv()

        qT[h] = qs[h].T

    def tri():
        r = lax.broadcasted_iota(jnp.int32, (tile, tile), 0)
        s = lax.broadcasted_iota(jnp.int32, (tile, tile), 1)
        return s >= r

    def span(t, kind):
        if kind == DIAG:
            return (t + 1) * tile
        return half if kind == SIB and (t + 1) * tile <= half else chip_len

    def cols(t):
        return slice(t * tile, (t + 1) * tile)

    def masked(s, t, kind, fill):
        nk = span(t, kind)
        if kind == DIAG:
            low = jnp.where(tri(), s[nk - tile:], fill)
            return jnp.concatenate([s[:nk - tile], low], axis=0) if nk > tile else low
        if kind == SIB:
            row = lax.broadcasted_iota(jnp.int32, (1, tile), 1) + t * tile
            seen = m * half + jnp.where(row >= half, half, 0)
            return jnp.where(lax.broadcasted_iota(jnp.int32, s.shape, 0) < seen, s, fill)
        return s

    def put_scores(t, kind, s):
        s = masked(s, t, kind, -jnp.inf)
        sb[:span(t, kind), cols(t)] = s
        mbr[:, cols(t)] = jnp.max(s, axis=0, keepdims=True)

    def scores(b, h, t, kind):
        return dot(kvs[b, 0, :span(t, kind), :], qT[h, :, cols(t)])

    def start_scores(b, h, kind):
        for t in range(n_tiles):
            put_scores(t, kind, scores(b, h, t, kind))

    def fwd_step(b, h, kind, bn, hn, kind_n):
        for t in range(n_tiles):
            sl = cols(t)
            nk = span(t, kind)
            top = mbr[:, sl]
            if kind != DIAG:
                old = mr[h, :, sl]
                top = jnp.maximum(old, top)
                fade = jnp.exp2((old - top) * c2)
            s = sb[:nk, sl]
            sn = scores(bn, hn, t, kind_n)
            p = jnp.exp2((s - top) * c2)
            tot = jnp.sum(p, axis=0, keepdims=True)
            o = dot(vT[b, :, :nk], p.astype(BF))
            put_scores(t, kind_n, sn)
            if kind == DIAG:
                lr[h, :, sl] = tot
                oT[h, :, sl] = o
            else:
                lr[h, :, sl] = lr[h, :, sl] * fade + tot
                oT[h, :, sl] = oT[h, :, sl] * fade + o
            mr[h, :, sl] = top

    def fwd_part(part):
        own = part == 0
        zq = jnp.where(own, z, zs)
        h0 = jnp.where(own, 0, heads)
        nh = jnp.where(own, n_own, take)
        cb = 2 * zq + m
        sbk = 2 * zq + 1 - m

        def fwd_block(i):
            b = 2 * (zq - 1 - i // 2) + jnp.where(lax.rem(i, 2) == 0, m, 1 - m)
            return jnp.where(i >= 2 * zq, cb, b)

        def arrive(i):
            b = fwd_block(i)
            p = zq - 1 - i // 2

            @pl.when(both(i < 2 * zq, either(own, p > z)))
            def _():
                column = lax.rem(i, 2) == 0
                relayed = both(between, column, p < z)

                @pl.when(jnp.logical_not(relayed))
                def _():
                    kv_wait(b)

                @pl.when(both(jnp.logical_not(relayed), column))
                def _():
                    kv_fwd(jnp.maximum(p, 0)).start()

                prep_kv(b)

        def plane(n):
            h = h0 + n

            @pl.when(n + 1 < nh)
            def _():
                prep_q(h + 1)

            @pl.when(both(own, n == RELAY1))
            def _():
                relay(1)

            if EXTRA:
                @pl.when(both(own, n == RELAY1))
                def _():
                    loop(give, give_all)

                @pl.when(both(own, n == n_own - 1))
                def _():
                    loop(give, give_all_d)

            fwd_step(cb, h, DIAG, sbk, h, SIB)
            fwd_step(sbk, h, SIB, cb, h0 + jnp.minimum(n + 1, nh - 1), DIAG)

        def full(n):
            i = n // nh
            k = n - i * nh
            last = k == nh - 1

            @pl.when(both(own, n == RELAY2))
            def _():
                relay(2)

            @pl.when(last)
            def _():
                arrive(i + 1)

            fwd_step(fwd_block(i), h0 + k, FULL, fwd_block(jnp.where(last, i + 1, i)), h0 + jnp.where(last, 0, k + 1), FULL)

        @pl.when(nh > 0)
        def _():
            @pl.when(jnp.logical_not(own))
            def _():
                kv_wait(cb)
                kv_fwd(zq).start()
                prep_kv(cb)

            prep_q(h0)
            start_scores(cb, h0, DIAG)
            kv_wait(sbk)
            prep_kv(sbk)
            loop(nh, plane)

            @pl.when(zq > 0)
            def _():
                arrive(0)
                start_scores(fwd_block(0), h0, FULL)
                loop(2 * zq * nh, full)

    loop(2 if EXTRA else 1, fwd_part)

    q_loc[1].wait()

    def slot(n):
        return jnp.where(n < n_own, n, n - n_own + heads)

    def fwd_end(n):
        h = slot(n)

        @pl.when(h < heads)
        def _():
            d_swap(jnp.minimum(h, heads - 1)).wait_recv()

        if EXTRA:
            @pl.when(h >= heads)
            def _():
                for r in (0, 1):
                    d_give(jnp.maximum(h - heads, 0), r).wait_recv()

        d = dos[h].T
        doT[h] = d
        l = lr[h]
        o = oT[h] / l
        mr[h] = mr[h] * c2 + jnp.log2(l)
        dr[h] = jnp.sum(o * d.astype(F32), axis=0, keepdims=True)
        os[h] = o.T.astype(BF)
        dqT[h] = jnp.zeros_like(o)

    loop(n_own + take, fwd_end)

    def res_copies(src, dst, loc, snd, rcv, h):
        return (pltpu.make_async_copy(src.at[h, my_rows], dst.at[y, h], loc.at[h]),
                rcopy(src.at[h, peer_rows], dst.at[y, h], snd.at[h], rcv.at[h], peer))

    def o_copies(h):
        return res_copies(os, o_out, o_loc, o_snd, o_rcv, h)

    def dq_copies(h):
        return res_copies(dqs, dq_out, dq_loc, dq_snd, dq_rcv, h)

    def back(src, dst, snd, rcv, j, r, n):
        return rcopy(src.at[heads + j, rows[r]], dst.at[y, heads - n + j], snd.at[j, r], rcv.at[j, r], mates[r])

    def start_both(pair):
        for cp in pair:
            cp.start()

    loop(n_own, lambda h: start_both(o_copies(h)))
    loop(take, lambda j: start_both(back(os, o_out, ho_snd, ho_rcv, j, r, take) for r in (0, 1)))

    def bwd_step(b, h, kind):
        for t in range(n_tiles):
            sl = cols(t)
            nk = span(t, kind)
            s = dot(kvs[b, 0, :nk, :], qT[h, :, sl])
            dp = dot(kvs[b, 1, :nk, :], doT[h, :, sl])
            p = masked(jnp.exp2(s * c2 - mr[h, :, sl]), t, kind, 0.0)
            ds = (p * (dp - dr[h, :, sl])).astype(BF)
            dkv[b, 1, :nk, :] += dot(p.astype(BF), dos[h, sl, :])
            dkv[b, 0, :nk, :] += dot(ds, qs[h, sl, :])
            dqT[h, :, sl] += dot(kT[b, :, :nk], ds)

    def y_send(p):
        return rcopy(dkv.at[2 * p + 1 - m], ybuf.at[p], y_snd.at[p], y_rcv.at[p], sib)

    def y_add(p):
        rcopy(dkv.at[0], ybuf.at[p], y_snd.at[p], y_rcv.at[p], sib).wait_recv()
        dkv[2 * p + m] = dkv[2 * p + m] + ybuf[p]

    def z_send(p):
        return rcopy(dkv.at[2 * p + m], zbuf.at[z], z_snd.at[p], z_rcv.at[z], {"ctxo": p})

    def c_send(p):
        return rcopy(dkv.at[2 * p + m], cbuf.at[p], z_snd.at[p], c_rcv.at[p], {"ctxo": 2})

    def leave(p):
        @pl.when(both(z == 3, p < 2))
        def _():
            c_send(jnp.minimum(p, 1)).start()

        @pl.when(either(both(z == 3, p == 2), z < 2))
        def _():
            z_send(p).start()

    def chain(p):
        rcopy(dkv.at[0], cbuf.at[p], z_snd.at[p], c_rcv.at[p], {"ctxo": 2}).wait_recv()
        dkv[2 * p + m] = dkv[2 * p + m] + cbuf[p]
        z_send(p).start()

    def finish_dq(h):
        dqs[h] = (dqT[h] * scale).T.astype(BF)

    n_planes = jnp.where(helps, zs, z)

    def bwd_full(i):
        k = i // 2
        p = jnp.where(helps, jnp.where(k == 0, 2, k - 1), k)
        first = lax.rem(i, 2) == 0
        b = 2 * p + jnp.where(first, 1 - m, m)
        na = jnp.where(p < z, n_own, 0)
        nb = take

        def one(n):
            bwd_step(b, jnp.where(n < na, n, n - na + heads), FULL)

        loop(na + nb, one)

        @pl.when(both(first, p != z))
        def _():
            y_send(p).start()

        if EXTRA:
            @pl.when(both(helps, i == 0))
            def _():
                y_add(zs)
                leave(zs)

        @pl.when(both(jnp.logical_not(first), p != z))
        def _():
            y_add(p)
            leave(p)

        @pl.when(both(z == 2, i == 2))
        def _():
            chain(0)

    def bwd_part(part):
        own = part == 1
        zq = jnp.where(own, z, zs)
        h0 = jnp.where(own, 0, heads)

        def plane(n):
            h = h0 + n
            bwd_step(2 * zq + 1 - m, h, SIB)
            bwd_step(2 * zq + m, h, DIAG)

            @pl.when(own)
            def _():
                finish_dq(h)

                @pl.when(h > 0)
                def _():
                    start_both(dq_copies(jnp.clip(h - 1, 0, heads - 1)))

                @pl.when(both(z == 2, h == 1))
                def _():
                    chain(1)

        loop(jnp.where(own, n_own, take), plane)

        @pl.when(either(own, helps))
        def _():
            y_send(zq).start()

        @pl.when(jnp.logical_not(own))
        def _():
            loop(2 * n_planes, bwd_full)

            def taken_dq(j):
                finish_dq(heads + j)

            loop(take, taken_dq)
            loop(take, lambda j: start_both(back(dqs, dq_out, hg_snd, hg_rcv, j, r, take) for r in (0, 1)))

    loop(2, bwd_part)
    start_both(dq_copies(n_own - 1))

    def z_comes(t):
        if t == 3:
            return z == 2
        if t == 2:
            return z < 2
        if t == 1:
            return z != 1 if EXTRA else z == 0
        return z < 0

    for t in range(nz):
        @pl.when(z_comes(t))
        def _():
            rcopy(dkv.at[0], zbuf.at[t], z_snd.at[0], z_rcv.at[t], {"ctxo": t}).wait_recv()
            dkv[c] = dkv[c] + zbuf[t]

    y_add(z)
    gs[0] = (dkv[c, 0] * scale).astype(BF)
    gs[1] = dkv[c, 1].astype(BF)
    outs = (dk_out, dv_out)
    g_copies = []
    for i in (0, 1):
        g_copies.append((pltpu.make_async_copy(gs.at[i, my_rows], outs[i].at[y], g_loc.at[i]),
                         rcopy(gs.at[i, peer_rows], outs[i].at[y], g_snd.at[i], g_rcv.at[i], peer)))
        start_both(g_copies[-1])

    for i in (0, 1):
        kv_swap(i)[0].wait_send()

    def own_sent(h):
        q_swap(h).wait_send()
        d_swap(h).wait_send()
        for a, b in (o_copies(h), dq_copies(h)):
            a.wait()
            b.wait()

    loop(n_own, own_sent)

    def given(j):
        for r in (0, 1):
            q_give(j, r).wait_send()
            d_give(j, r).wait_send()
            for dst, snd, rcv in ((o_out, ho_snd, ho_rcv), (dq_out, hg_snd, hg_rcv)):
                rcopy(os.at[0, my_rows], dst.at[batch[r], heads - give + j], snd.at[j, r], rcv.at[j, r], mates[r]).wait_recv()

    def taken(j):
        for r in (0, 1):
            back(os, o_out, ho_snd, ho_rcv, j, r, take).wait_send()
            back(dqs, dq_out, hg_snd, hg_rcv, j, r, take).wait_send()

    if EXTRA:
        loop(give, given)
        loop(take, taken)

    @pl.when(z < nz - 1)
    def _():
        loop(z + 1, lambda p: kv_up(p).wait_send())

    if EXTRA:
        @pl.when(z >= 2)
        def _():
            loop(nz - z, lambda k: kv_down(z + k).wait_send())

    def planes_sent(p):
        kv_fwd(p).wait_send()
        y_send(p).wait_send()

        @pl.when(p != z)
        def _():
            z_send(p).wait_send()

    loop(jnp.where(helps, zs, z) + 1, planes_sent)
    for a, b in g_copies:
        a.wait()
        b.wait()


def hand_over(*refs):
    srcs, dsts, bufs, came, left = refs[:4], refs[4:8], refs[8:12], refs[12], refs[13]
    parts = [(i, b) for i in range(4) for b in range(srcs[0].shape[0])]
    ins = [pltpu.make_async_copy(srcs[i].at[b], bufs[i].at[b], came.at[n]) for n, (i, b) in enumerate(parts)]
    outs = [pltpu.make_async_copy(bufs[i].at[b], dsts[i].at[b], left.at[n]) for n, (i, b) in enumerate(parts)]
    for cp in ins:
        cp.start()
    for a, b in zip(ins, outs):
        a.wait()
        b.start()
    for cp in outs:
        cp.wait()


def solution(mesh):
    nz = mesh.shape["ctxo"]
    spec = P("data", ("ctxo", "ctx"), None, None)

    def local(q, k, v, do):
        rows, half, heads, dim = q.shape
        n = 2 * half
        nb = 2 * nz
        nh = heads + EXTRA
        ex = max(EXTRA, 1)
        q, do = jnp.swapaxes(q, 1, 2), jnp.swapaxes(do, 1, 2)
        k, v = k[:, :, 0], v[:, :, 0]
        hbm = pl.BlockSpec(memory_space=pl.ANY)
        S = jax.ShapeDtypeStruct
        V = pltpu.VMEM

        def dma(*shape):
            return pltpu.SemaphoreType.DMA(shape)

        o, dq, dk, dv = pl.pallas_call(
            functools.partial(kernel, heads),
            out_shape=[S(q.shape, BF), S(q.shape, BF), S(k.shape, BF), S(k.shape, BF)],
            in_specs=[hbm] * 4,
            out_specs=[hbm] * 4,
            scratch_shapes=[
                V((nh, n, dim), BF), V((nh, n, dim), BF), V((nh, dim, n), BF), V((nh, dim, n), BF),
                V((nb, 2, n, dim), BF), V((nb, dim, n), BF), V((nb, dim, n), BF),
                V((nh, dim, n), F32), V((nh, dim, n), F32),
                V((nh, 1, n), F32), V((nh, 1, n), F32), V((nh, 1, n), F32),
                V((n, n), F32), V((1, n), F32),
                V((nb, 2, n, dim), F32), V((nz, 2, n, dim), F32), V((nz, 2, n, dim), F32), V((2, 2, n, dim), F32),
                V((nh, n, dim), BF), V((nh, n, dim), BF), V((2, n, dim), BF),
                dma(2), dma(2), dma(2), dma(2), dma(heads), dma(heads), dma(heads), dma(heads),
                dma(ex, 2), dma(ex, 2), dma(ex, 2), dma(ex, 2),
                dma(nz), dma(nz), dma(nz), dma(nb), dma(nz), dma(nz), dma(nz), dma(nz), dma(2),
                dma(heads), dma(heads), dma(heads), dma(heads), dma(heads), dma(heads),
                dma(ex, 2), dma(ex, 2), dma(ex, 2), dma(ex, 2), dma(2), dma(2), dma(2),
            ],
            compiler_params=pltpu.CompilerParams(collective_id=0, has_side_effects=True, vmem_limit_bytes=62 * 1024 * 1024),
            name="attn",
        )(q, do, k, v)
        o, dq, dk, dv = pl.pallas_call(
            hand_over,
            out_shape=[S(t.shape, BF) for t in (o, dq, dk, dv)],
            in_specs=[hbm] * 4,
            out_specs=[hbm] * 4,
            scratch_shapes=[V(t.shape, BF) for t in (o, dq, dk, dv)] + [dma(4 * rows), dma(4 * rows)],
            name="hand_over",
        )(o, dq, dk, dv)
        return jnp.swapaxes(o, 1, 2), jnp.swapaxes(dq, 1, 2), dk[:, :, None], dv[:, :, None]

    return jax.shard_map(local, mesh=mesh, in_specs=(spec,) * 4, out_specs=(spec,) * 4, check_vma=False)
```

```python
import functools
import math

import jax
import jax.numpy as jnp
from jax import lax
from jax.experimental import pallas as pl
from jax.experimental.pallas import tpu as pltpu
from jax.sharding import PartitionSpec as P

MESH = pl.DeviceIdType.MESH
BF = jnp.bfloat16
F32 = jnp.float32
DIAG, SIB, FULL = 0, 1, 2
EXTRA = 1
RELAY1, RELAY2 = 3, 4


def dot(a, b):
    return jnp.dot(a, b, preferred_element_type=F32)


def either(*conds):
    return functools.reduce(jnp.logical_or, conds)


def both(*conds):
    return functools.reduce(jnp.logical_and, conds)


def loop(n, body):
    def step(i, carry):
        body(i)
        return carry

    lax.fori_loop(0, n, step, 0)


def kernel(heads, q_in, do_in, k_in, v_in, o_out, dq_out, dk_out, dv_out,
           qs, dos, qT, doT, kvs, kT, vT, oT, dqT, mr, lr, dr, sb, mbr, dkv, ybuf, zbuf, cbuf, os, dqs, gs,
           kv_loc, kv_snd, kv_xrc, qd_loc, q_snd, q_rcv, d_snd, d_rcv, hq_snd, hq_rcv, hd_snd, hd_rcv,
           kv_us, kv_ds, kv_fs, kv_rcv, y_snd, y_rcv, z_snd, z_rcv, c_rcv,
           o_loc, o_snd, o_rcv, dq_loc, dq_snd, dq_rcv, ho_snd, ho_rcv, hg_snd, hg_rcv, g_loc, g_snd, g_rcv):
    _, chip_len, dim = qs.shape
    nz = 4
    half = chip_len // 2
    tile = min(256, chip_len)
    n_tiles = chip_len // tile
    scale = 1.0 / math.sqrt(dim)
    c2 = scale * math.log2(math.e)

    z = lax.axis_index("ctxo")
    x = lax.axis_index("ctx")
    m = lax.rem(x, 2)
    y = x // 2
    zs = lax.rem(z + 2, nz)
    give = jnp.where(z == 3, EXTRA, 0)
    take = jnp.where(z == 1, EXTRA, 0)
    n_own = heads - give
    helps = take > 0
    c = 2 * z + m
    peer = {"ctx": 2 * (1 - y) + m}
    sib = {"ctx": 2 * y + 1 - m}
    mates = ({"ctxo": zs}, {"ctxo": zs, "ctx": 2 * (1 - y) + m})
    my_rows = pl.ds(pl.multiple_of(y * half, half), half)
    peer_rows = pl.ds(pl.multiple_of((1 - y) * half, half), half)
    batch = (y, 1 - y)
    rows = (my_rows, peer_rows)

    def rcopy(src, dst, ss, rs, dev):
        return pltpu.make_async_remote_copy(src_ref=src, dst_ref=dst, send_sem=ss, recv_sem=rs, device_id=dev, device_id_type=MESH)

    bar = pltpu.get_barrier_semaphore()
    for dev in (peer, sib, mates[1]) + tuple({"ctxo": lax.rem(z + d, nz)} for d in range(1, nz)):
        pl.semaphore_signal(bar, inc=1, device_id=dev, device_id_type=MESH)
    pl.semaphore_wait(bar, nz + 2)

    def kv_swap(i):
        src = (k_in, v_in)[i]
        return (rcopy(src.at[1 - y], kvs.at[c, i, my_rows], kv_snd.at[i], kv_xrc.at[i], peer),
                pltpu.make_async_copy(src.at[y], kvs.at[c, i, my_rows], kv_loc.at[i]))

    def q_swap(h):
        return rcopy(q_in.at[1 - y, h], qs.at[h, my_rows], q_snd.at[h], q_rcv.at[h], peer)

    def d_swap(h):
        return rcopy(do_in.at[1 - y, h], dos.at[h, my_rows], d_snd.at[h], d_rcv.at[h], peer)

    def q_give(j, r):
        return rcopy(q_in.at[batch[r], jnp.minimum(heads - give + j, heads - 1)], qs.at[heads + j, my_rows], hq_snd.at[j, r], hq_rcv.at[j, r], mates[r])

    def d_give(j, r):
        return rcopy(do_in.at[batch[r], jnp.minimum(heads - give + j, heads - 1)], dos.at[heads + j, my_rows], hd_snd.at[j, r], hd_rcv.at[j, r], mates[r])

    for i in (0, 1):
        for cp in kv_swap(i):
            cp.start()
    q_loc = (pltpu.make_async_copy(q_in.at[y], qs.at[:heads, my_rows], qd_loc.at[0]),
             pltpu.make_async_copy(do_in.at[y], dos.at[:heads, my_rows], qd_loc.at[1]))
    for cp in q_loc:
        cp.start()
    dkv[...] = jnp.zeros_like(dkv)
    for i in (0, 1):
        swap, local = kv_swap(i)
        local.wait()
        swap.wait_recv()
    for h in (0, 1, 2):
        q_swap(h).start()

    def kv_up(p):
        b = 2 * p + m
        return rcopy(kvs.at[b], kvs.at[b], kv_us.at[p], kv_rcv.at[b], {"ctxo": jnp.minimum(z + 1, nz - 1)})

    def kv_down(p):
        b = 2 * p + m
        return rcopy(kvs.at[b], kvs.at[b], kv_ds.at[p], kv_rcv.at[b], {"ctxo": jnp.maximum(z - 1, 0)})

    def kv_fwd(p):
        b = 2 * p + m
        return rcopy(kvs.at[b], kvs.at[b], kv_fs.at[p], kv_rcv.at[b], sib)

    def kv_wait(b):
        rcopy(kvs.at[b], kvs.at[b], kv_fs.at[0], kv_rcv.at[b], sib).wait_recv()

    kv_fwd(z).start()
    @pl.when(z < nz - 1)
    def _():
        kv_up(z).start()

    if EXTRA:
        @pl.when(z >= 2)
        def _():
            kv_down(z).start()

    between = both(z > 0, z < nz - 1)

    def relay(r):
        lo, hi = z - r, z + r

        @pl.when(both(between, lo >= 0))
        def _():
            p = jnp.maximum(lo, 0)
            kv_wait(2 * p + m)
            kv_up(p).start()
            kv_fwd(p).start()

        if EXTRA:
            @pl.when(both(z == 2, hi < nz))
            def _():
                p = jnp.minimum(hi, nz - 1)
                kv_wait(2 * p + m)
                kv_down(p).start()

    def give_all(j):
        for r in (0, 1):
            q_give(j, r).start()

    def give_all_d(j):
        for r in (0, 1):
            d_give(j, r).start()

    def prep_kv(b):
        kT[b] = kvs[b, 0].T
        vT[b] = kvs[b, 1].T

    prep_kv(c)
    q_loc[0].wait()

    def prep_q(h):
        @pl.when(h < heads)
        def _():
            q_swap(jnp.minimum(h, heads - 1)).wait_recv()

            @pl.when(h + 3 < n_own)
            def _():
                q_swap(jnp.minimum(h + 3, heads - 1)).start()

            @pl.when(h + 2 == n_own)
            def _():
                loop(n_own, lambda k: d_swap(k).start())

        if EXTRA:
            @pl.when(h >= heads)
            def _():
                for r in (0, 1):
                    q_give(jnp.maximum(h - heads, 0), r).wait_recv()

        qT[h] = qs[h].T

    def tri():
        r = lax.broadcasted_iota(jnp.int32, (tile, tile), 0)
        s = lax.broadcasted_iota(jnp.int32, (tile, tile), 1)
        return s >= r

    def span(t, kind):
        if kind == DIAG:
            return (t + 1) * tile
        return half if kind == SIB and (t + 1) * tile <= half else chip_len

    def cols(t):
        return slice(t * tile, (t + 1) * tile)

    def masked(s, t, kind, fill):
        nk = span(t, kind)
        if kind == DIAG:
            low = jnp.where(tri(), s[nk - tile:], fill)
            return jnp.concatenate([s[:nk - tile], low], axis=0) if nk > tile else low
        if kind == SIB:
            row = lax.broadcasted_iota(jnp.int32, (1, tile), 1) + t * tile
            seen = m * half + jnp.where(row >= half, half, 0)
            return jnp.where(lax.broadcasted_iota(jnp.int32, s.shape, 0) < seen, s, fill)
        return s

    def put_scores(t, kind, s):
        s = masked(s, t, kind, -jnp.inf)
        sb[:span(t, kind), cols(t)] = s
        mbr[:, cols(t)] = jnp.max(s, axis=0, keepdims=True)

    def scores(b, h, t, kind):
        return dot(kvs[b, 0, :span(t, kind), :], qT[h, :, cols(t)])

    def start_scores(b, h, kind):
        for t in range(n_tiles):
            put_scores(t, kind, scores(b, h, t, kind))

    def fwd_step(b, h, kind, bn, hn, kind_n):
        for t in range(n_tiles):
            sl = cols(t)
            nk = span(t, kind)
            top = mbr[:, sl]
            if kind != DIAG:
                old = mr[h, :, sl]
                top = jnp.maximum(old, top)
                fade = jnp.exp2((old - top) * c2)
            s = sb[:nk, sl]
            sn = scores(bn, hn, t, kind_n)
            p = jnp.exp2((s - top) * c2)
            tot = jnp.sum(p, axis=0, keepdims=True)
            o = dot(vT[b, :, :nk], p.astype(BF))
            put_scores(t, kind_n, sn)
            if kind == DIAG:
                lr[h, :, sl] = tot
                oT[h, :, sl] = o
            else:
                lr[h, :, sl] = lr[h, :, sl] * fade + tot
                oT[h, :, sl] = oT[h, :, sl] * fade + o
            mr[h, :, sl] = top

    def fwd_part(part):
        own = part == 0
        zq = jnp.where(own, z, zs)
        h0 = jnp.where(own, 0, heads)
        nh = jnp.where(own, n_own, take)
        cb = 2 * zq + m
        sbk = 2 * zq + 1 - m

        def fwd_block(i):
            b = 2 * (zq - 1 - i // 2) + jnp.where(lax.rem(i, 2) == 0, m, 1 - m)
            return jnp.where(i >= 2 * zq, cb, b)

        def arrive(i):
            b = fwd_block(i)
            p = zq - 1 - i // 2

            @pl.when(both(i < 2 * zq, either(own, p > z)))
            def _():
                column = lax.rem(i, 2) == 0
                relayed = both(between, column, p < z)

                @pl.when(jnp.logical_not(relayed))
                def _():
                    kv_wait(b)

                @pl.when(both(jnp.logical_not(relayed), column))
                def _():
                    kv_fwd(jnp.maximum(p, 0)).start()

                prep_kv(b)

        def plane(n):
            h = h0 + n

            @pl.when(n + 1 < nh)
            def _():
                prep_q(h + 1)

            @pl.when(both(own, n == RELAY1))
            def _():
                relay(1)

            if EXTRA:
                @pl.when(both(own, n == RELAY1))
                def _():
                    loop(give, give_all)

                @pl.when(both(own, n == n_own - 1))
                def _():
                    loop(give, give_all_d)

            fwd_step(cb, h, DIAG, sbk, h, SIB)
            fwd_step(sbk, h, SIB, cb, h0 + jnp.minimum(n + 1, nh - 1), DIAG)

        def full(n):
            i = n // nh
            k = n - i * nh
            last = k == nh - 1

            @pl.when(both(own, n == RELAY2))
            def _():
                relay(2)

            @pl.when(last)
            def _():
                arrive(i + 1)

            fwd_step(fwd_block(i), h0 + k, FULL, fwd_block(jnp.where(last, i + 1, i)), h0 + jnp.where(last, 0, k + 1), FULL)

        @pl.when(nh > 0)
        def _():
            @pl.when(jnp.logical_not(own))
            def _():
                kv_wait(cb)
                kv_fwd(zq).start()
                prep_kv(cb)

            prep_q(h0)
            start_scores(cb, h0, DIAG)
            kv_wait(sbk)
            prep_kv(sbk)
            loop(nh, plane)

            @pl.when(zq > 0)
            def _():
                arrive(0)
                start_scores(fwd_block(0), h0, FULL)
                loop(2 * zq * nh, full)

    loop(2 if EXTRA else 1, fwd_part)

    q_loc[1].wait()

    def slot(n):
        return jnp.where(n < n_own, n, n - n_own + heads)

    def fwd_end(n):
        h = slot(n)

        @pl.when(h < heads)
        def _():
            d_swap(jnp.minimum(h, heads - 1)).wait_recv()

        if EXTRA:
            @pl.when(h >= heads)
            def _():
                for r in (0, 1):
                    d_give(jnp.maximum(h - heads, 0), r).wait_recv()

        d = dos[h].T
        doT[h] = d
        l = lr[h]
        o = oT[h] / l
        mr[h] = mr[h] * c2 + jnp.log2(l)
        dr[h] = jnp.sum(o * d.astype(F32), axis=0, keepdims=True)
        os[h] = o.T.astype(BF)
        dqT[h] = jnp.zeros_like(o)

    loop(n_own + take, fwd_end)

    def res_copies(src, dst, loc, snd, rcv, h):
        return (pltpu.make_async_copy(src.at[h, my_rows], dst.at[y, h], loc.at[h]),
                rcopy(src.at[h, peer_rows], dst.at[y, h], snd.at[h], rcv.at[h], peer))

    def o_copies(h):
        return res_copies(os, o_out, o_loc, o_snd, o_rcv, h)

    def dq_copies(h):
        return res_copies(dqs, dq_out, dq_loc, dq_snd, dq_rcv, h)

    def back(src, dst, snd, rcv, j, r, n):
        return rcopy(src.at[heads + j, rows[r]], dst.at[y, heads - n + j], snd.at[j, r], rcv.at[j, r], mates[r])

    def start_both(pair):
        for cp in pair:
            cp.start()

    loop(n_own, lambda h: start_both(o_copies(h)))
    loop(take, lambda j: start_both(back(os, o_out, ho_snd, ho_rcv, j, r, take) for r in (0, 1)))

    def bwd_step(b, h, kind):
        for t in range(n_tiles):
            sl = cols(t)
            nk = span(t, kind)
            s = dot(kvs[b, 0, :nk, :], qT[h, :, sl])
            dp = dot(kvs[b, 1, :nk, :], doT[h, :, sl])
            p = masked(jnp.exp2(s * c2 - mr[h, :, sl]), t, kind, 0.0)
            ds = (p * (dp - dr[h, :, sl])).astype(BF)
            dkv[b, 1, :nk, :] += dot(p.astype(BF), dos[h, sl, :])
            dkv[b, 0, :nk, :] += dot(ds, qs[h, sl, :])
            dqT[h, :, sl] += dot(kT[b, :, :nk], ds)

    def y_send(p):
        return rcopy(dkv.at[2 * p + 1 - m], ybuf.at[p], y_snd.at[p], y_rcv.at[p], sib)

    def y_add(p):
        rcopy(dkv.at[0], ybuf.at[p], y_snd.at[p], y_rcv.at[p], sib).wait_recv()
        dkv[2 * p + m] = dkv[2 * p + m] + ybuf[p]

    def z_send(p):
        return rcopy(dkv.at[2 * p + m], zbuf.at[z], z_snd.at[p], z_rcv.at[z], {"ctxo": p})

    def c_send(p):
        return rcopy(dkv.at[2 * p + m], cbuf.at[p], z_snd.at[p], c_rcv.at[p], {"ctxo": 2})

    def leave(p):
        @pl.when(both(z == 3, p < 2))
        def _():
            c_send(jnp.minimum(p, 1)).start()

        @pl.when(either(both(z == 3, p == 2), z < 2))
        def _():
            z_send(p).start()

    def chain(p):
        rcopy(dkv.at[0], cbuf.at[p], z_snd.at[p], c_rcv.at[p], {"ctxo": 2}).wait_recv()
        dkv[2 * p + m] = dkv[2 * p + m] + cbuf[p]
        z_send(p).start()

    def finish_dq(h):
        dqs[h] = (dqT[h] * scale).T.astype(BF)

    n_planes = jnp.where(helps, zs, z)

    def bwd_full(i):
        k = i // 2
        p = jnp.where(helps, jnp.where(k == 0, 2, k - 1), k)
        first = lax.rem(i, 2) == 0
        b = 2 * p + jnp.where(first, 1 - m, m)
        na = jnp.where(p < z, n_own, 0)
        nb = take

        def one(n):
            bwd_step(b, jnp.where(n < na, n, n - na + heads), FULL)

        loop(na + nb, one)

        @pl.when(both(first, p != z))
        def _():
            y_send(p).start()

        if EXTRA:
            @pl.when(both(helps, i == 0))
            def _():
                y_add(zs)
                leave(zs)

        @pl.when(both(jnp.logical_not(first), p != z))
        def _():
            y_add(p)
            leave(p)

        @pl.when(both(z == 2, i == 2))
        def _():
            chain(0)

    def bwd_part(part):
        own = part == 1
        zq = jnp.where(own, z, zs)
        h0 = jnp.where(own, 0, heads)

        def plane(n):
            h = h0 + n
            bwd_step(2 * zq + 1 - m, h, SIB)
            bwd_step(2 * zq + m, h, DIAG)

            @pl.when(own)
            def _():
                finish_dq(h)

                @pl.when(h > 0)
                def _():
                    start_both(dq_copies(jnp.clip(h - 1, 0, heads - 1)))

                @pl.when(both(z == 2, h == 1))
                def _():
                    chain(1)

        loop(jnp.where(own, n_own, take), plane)

        @pl.when(either(own, helps))
        def _():
            y_send(zq).start()

        @pl.when(jnp.logical_not(own))
        def _():
            loop(2 * n_planes, bwd_full)

            def taken_dq(j):
                finish_dq(heads + j)

            loop(take, taken_dq)
            loop(take, lambda j: start_both(back(dqs, dq_out, hg_snd, hg_rcv, j, r, take) for r in (0, 1)))

    loop(2, bwd_part)
    start_both(dq_copies(n_own - 1))

    def z_comes(t):
        if t == 3:
            return z == 2
        if t == 2:
            return z < 2
        if t == 1:
            return z != 1 if EXTRA else z == 0
        return z < 0

    for t in range(nz):
        @pl.when(z_comes(t))
        def _():
            rcopy(dkv.at[0], zbuf.at[t], z_snd.at[0], z_rcv.at[t], {"ctxo": t}).wait_recv()
            dkv[c] = dkv[c] + zbuf[t]

    y_add(z)
    gs[0] = (dkv[c, 0] * scale).astype(BF)
    gs[1] = dkv[c, 1].astype(BF)
    outs = (dk_out, dv_out)
    g_copies = []
    for i in (0, 1):
        g_copies.append((pltpu.make_async_copy(gs.at[i, my_rows], outs[i].at[y], g_loc.at[i]),
                         rcopy(gs.at[i, peer_rows], outs[i].at[y], g_snd.at[i], g_rcv.at[i], peer)))
        start_both(g_copies[-1])

    for i in (0, 1):
        kv_swap(i)[0].wait_send()

    def own_sent(h):
        q_swap(h).wait_send()
        d_swap(h).wait_send()
        for a, b in (o_copies(h), dq_copies(h)):
            a.wait()
            b.wait()

    loop(n_own, own_sent)

    def given(j):
        for r in (0, 1):
            q_give(j, r).wait_send()
            d_give(j, r).wait_send()
            for dst, snd, rcv in ((o_out, ho_snd, ho_rcv), (dq_out, hg_snd, hg_rcv)):
                rcopy(os.at[0, my_rows], dst.at[batch[r], heads - give + j], snd.at[j, r], rcv.at[j, r], mates[r]).wait_recv()

    def taken(j):
        for r in (0, 1):
            back(os, o_out, ho_snd, ho_rcv, j, r, take).wait_send()
            back(dqs, dq_out, hg_snd, hg_rcv, j, r, take).wait_send()

    if EXTRA:
        loop(give, given)
        loop(take, taken)

    @pl.when(z < nz - 1)
    def _():
        loop(z + 1, lambda p: kv_up(p).wait_send())

    if EXTRA:
        @pl.when(z >= 2)
        def _():
            loop(nz - z, lambda k: kv_down(z + k).wait_send())

    def planes_sent(p):
        kv_fwd(p).wait_send()
        y_send(p).wait_send()

        @pl.when(p != z)
        def _():
            z_send(p).wait_send()

    loop(jnp.where(helps, zs, z) + 1, planes_sent)
    for a, b in g_copies:
        a.wait()
        b.wait()


def hand_over(*refs):
    srcs, dsts, bufs, came, left = refs[:4], refs[4:8], refs[8:12], refs[12], refs[13]
    parts = [(i, b) for i in range(4) for b in range(srcs[0].shape[0])]
    ins = [pltpu.make_async_copy(srcs[i].at[b], bufs[i].at[b], came.at[n]) for n, (i, b) in enumerate(parts)]
    outs = [pltpu.make_async_copy(bufs[i].at[b], dsts[i].at[b], left.at[n]) for n, (i, b) in enumerate(parts)]
    for cp in ins:
        cp.start()
    for a, b in zip(ins, outs):
        a.wait()
        b.start()
    for cp in outs:
        cp.wait()


def solution(mesh):
    nz = mesh.shape["ctxo"]
    spec = P("data", ("ctxo", "ctx"), None, None)

    def local(q, k, v, do):
        rows, half, heads, dim = q.shape
        n = 2 * half
        nb = 2 * nz
        nh = heads + EXTRA
        ex = max(EXTRA, 1)
        q, do = jnp.swapaxes(q, 1, 2), jnp.swapaxes(do, 1, 2)
        k, v = k[:, :, 0], v[:, :, 0]
        hbm = pl.BlockSpec(memory_space=pl.ANY)
        S = jax.ShapeDtypeStruct
        V = pltpu.VMEM

        def dma(*shape):
            return pltpu.SemaphoreType.DMA(shape)

        o, dq, dk, dv = pl.pallas_call(
            functools.partial(kernel, heads),
            out_shape=[S(q.shape, BF), S(q.shape, BF), S(k.shape, BF), S(k.shape, BF)],
            in_specs=[hbm] * 4,
            out_specs=[hbm] * 4,
            scratch_shapes=[
                V((nh, n, dim), BF), V((nh, n, dim), BF), V((nh, dim, n), BF), V((nh, dim, n), BF),
                V((nb, 2, n, dim), BF), V((nb, dim, n), BF), V((nb, dim, n), BF),
                V((nh, dim, n), F32), V((nh, dim, n), F32),
                V((nh, 1, n), F32), V((nh, 1, n), F32), V((nh, 1, n), F32),
                V((n, n), F32), V((1, n), F32),
                V((nb, 2, n, dim), F32), V((nz, 2, n, dim), F32), V((nz, 2, n, dim), F32), V((2, 2, n, dim), F32),
                V((nh, n, dim), BF), V((nh, n, dim), BF), V((2, n, dim), BF),
                dma(2), dma(2), dma(2), dma(2), dma(heads), dma(heads), dma(heads), dma(heads),
                dma(ex, 2), dma(ex, 2), dma(ex, 2), dma(ex, 2),
                dma(nz), dma(nz), dma(nz), dma(nb), dma(nz), dma(nz), dma(nz), dma(nz), dma(2),
                dma(heads), dma(heads), dma(heads), dma(heads), dma(heads), dma(heads),
                dma(ex, 2), dma(ex, 2), dma(ex, 2), dma(ex, 2), dma(2), dma(2), dma(2),
            ],
            compiler_params=pltpu.CompilerParams(collective_id=0, has_side_effects=True, vmem_limit_bytes=62 * 1024 * 1024),
            name="attn",
        )(q, do, k, v)
        o, dq, dk, dv = pl.pallas_call(
            hand_over,
            out_shape=[S(t.shape, BF) for t in (o, dq, dk, dv)],
            in_specs=[hbm] * 4,
            out_specs=[hbm] * 4,
            scratch_shapes=[V(t.shape, BF) for t in (o, dq, dk, dv)] + [dma(4 * rows), dma(4 * rows)],
            name="hand_over",
        )(o, dq, dk, dv)
        return jnp.swapaxes(o, 1, 2), jnp.swapaxes(dq, 1, 2), dk[:, :, None], dv[:, :, None]

    return jax.shard_map(local, mesh=mesh, in_specs=(spec,) * 4, out_specs=(spec,) * 4, check_vma=False)
```
